16 devices in a mesh: dp: 2 (over z), row: 2 (over y), fsdp: 4 (over x, core).
Axes of the slice: x: 2, y: 2, z: 2, core: 2. Of those that a mesh axis runs over, the one named last changes fastest.
Arguments:
- x_in: bfloat16 [65536, 576], P(('dp', 'row', 'fsdp'))
- dy_out: bfloat16 [65536, 576], P(('dp', 'row', 'fsdp'))
- w_gate: bfloat16 [576, 1536], P(None, ('row', 'fsdp'))
- w_up: bfloat16 [576, 1536], P(None, ('row', 'fsdp'))
- w_down: bfloat16 [1536, 576], P(('row', 'fsdp'))
- g_next: float32 [16, 3, 576, 1536], P(('dp', 'row', 'fsdp'))
Outputs:
- output 1: bfloat16 [65536, 576], P(('dp', 'row', 'fsdp'))
- output 2: float32 [3, 576, 1536], P(None, None, ('row', 'fsdp'))
- output 3: float32 [16, 3, 576, 1536], P(('dp', 'row', 'fsdp'))
All inputs are finite; a program needn't handle non-finite values.
Results may differ from the reference program's by a relative error of at most 0.0121358.
Values are sent between devices in bfloat16 or wider.
A program may use at most 1 GiB of HBM per device.

```python
import jax
import jax.numpy as jnp
from jax import lax
import math

MODEL_DIM = 576
HIDDEN_DIM = 1536
TOKENS_DEV = 4096
DEVICES = 16


def setup_inputs(seed: int = 0) -> dict:
    rand_keys = jax.random.split(jax.random.key(seed), 6)
    act_shape = (DEVICES * TOKENS_DEV, MODEL_DIM)
    in_scale = 1.0 / math.sqrt(MODEL_DIM)
    hid_scale = 1.0 / math.sqrt(HIDDEN_DIM)
    x_in = jax.random.normal(rand_keys[0], act_shape, jnp.float32).astype(jnp.bfloat16)
    dy_out = jax.random.normal(rand_keys[1], act_shape, jnp.float32).astype(jnp.bfloat16)
    w_gate = (jax.random.normal(rand_keys[2], (MODEL_DIM, HIDDEN_DIM), jnp.float32) * in_scale).astype(jnp.bfloat16)
    w_up = (jax.random.normal(rand_keys[3], (MODEL_DIM, HIDDEN_DIM), jnp.float32) * in_scale).astype(jnp.bfloat16)
    w_down = (jax.random.normal(rand_keys[4], (HIDDEN_DIM, MODEL_DIM), jnp.float32) * hid_scale).astype(jnp.bfloat16)
    g_next = jax.random.normal(rand_keys[5], (DEVICES, 3, MODEL_DIM, HIDDEN_DIM), jnp.float32)
    return {"x_in": x_in, "dy_out": dy_out, "w_gate": w_gate, "w_up": w_up, "w_down": w_down, "g_next": g_next}


def local_backward(x_blk, dy_blk, w_gate, w_up, w_down):
    a_pre = jnp.dot(x_blk, w_gate, preferred_element_type=jnp.float32)
    b_pre = jnp.dot(x_blk, w_up, preferred_element_type=jnp.float32)
    sig_a = jax.nn.sigmoid(a_pre)
    silu_a = a_pre * sig_a
    h_act = (silu_a * b_pre).astype(jnp.bfloat16)
    dh_full = jnp.dot(dy_blk, w_down.T, preferred_element_type=jnp.float32)
    da_bf = (dh_full * b_pre * sig_a * (1.0 + a_pre * (1.0 - sig_a))).astype(jnp.bfloat16)
    db_bf = (dh_full * silu_a).astype(jnp.bfloat16)
    dx_acc = jnp.dot(da_bf, w_gate.T, preferred_element_type=jnp.float32) + jnp.dot(db_bf, w_up.T, preferred_element_type=jnp.float32)
    grad_gate = jnp.dot(x_blk.T, da_bf, preferred_element_type=jnp.float32)
    grad_up = jnp.dot(x_blk.T, db_bf, preferred_element_type=jnp.float32)
    grad_down = jnp.dot(dy_blk.T, h_act, preferred_element_type=jnp.float32)
    return dx_acc.astype(jnp.bfloat16), jnp.stack([grad_gate, grad_up, grad_down])


def reference(x_in, dy_out, w_gate, w_up, w_down, g_next):
    x_blocks = x_in.reshape(DEVICES, TOKENS_DEV, MODEL_DIM)
    dy_blocks = dy_out.reshape(DEVICES, TOKENS_DEV, MODEL_DIM)

    def per_device(block_pair):
        return local_backward(block_pair[0], block_pair[1], w_gate, w_up, w_down)

    dx_blocks, dw_local = lax.map(per_device, (x_blocks, dy_blocks))
    dx_in = dx_blocks.reshape(DEVICES * TOKENS_DEV, MODEL_DIM)
    dw_next = jnp.sum(g_next.astype(jnp.bfloat16).astype(jnp.float32), axis=0)
    return (dx_in, dw_next, dw_local)
```

```python
import jax
import jax.numpy as jnp
from jax import lax
from jax.experimental import pallas as pl
from jax.experimental.pallas import tpu as pltpu
from jax.sharding import PartitionSpec as P

ALL_AXES = ("dp", "row", "fsdp")
GROUP_AXES = ("row", "fsdp")
MESH = pl.DeviceIdType.MESH
NN = (((1,), (0,)), ((), ()))
NT = (((1,), (1,)), ((), ()))
TN = (((0,), (0,)), ((), ()))
F32 = jnp.float32
BF = jnp.bfloat16
ANY = pl.BlockSpec(memory_space=pl.ANY)

D = 576
H = 1536
T = 4096
TA = 3072
TB = T - TA
CH = 144
BLK = 384
VMEM_LIMIT = 67043328
OWN_OUT, X_OUT, Y_OUT, OWN_MID, X_MID, Y_MID, DIAG = 0, 256, 512, 768, 896, 1024, 1152


def dot(lhs, rhs, dims):
    return lax.dot_general(lhs, rhs, dims, preferred_element_type=F32)


def forward_tile(x, dy, w, rows):
    a = dot(w[0, rows, :], x, NN)
    b = dot(w[1, rows, :], x, NN)
    dh = dot(w[2, rows, :], dy, NN)
    s = jax.nn.sigmoid(a)
    silu = a * s
    h = (silu * b).astype(BF)
    da = (dh * b * s * (1.0 + a * (1.0 - s))).astype(BF)
    db = (dh * silu).astype(BF)
    return h, da, db


def dx_tile(da, db, w, rows):
    return dot(w[0, rows, :], da, TN) + dot(w[1, rows, :], db, TN)


def kernel_a(
    x_hbm, dy_hbm, w1_hbm, w3_hbm, w2_hbm, g_hbm,
    w_out, dw_out, dx_out, sum_out,
    xv, dv, w, da_s, db_s, h_s, dxa, dxo, dwo,
    stage, part, r0, acc, rz, r1, kept, r2, own, theirs,
    in_sem, wl_sem, ws, wr, st_sem, p_s, p_r, z_s, z_r, d1_s, d1_r, d2_s, d2_r, za_s, za_r, f_s, f_r, dxo_sem, dwo_sem, out_sem,
):
    dp = lax.axis_index("dp")
    row = lax.axis_index("row")
    f = lax.axis_index("fsdp")
    c = lax.rem(f, 2)
    x = f // 2
    fx = lax.rem(f + 2, 4)
    to_core = {"fsdp": f + 1 - 2 * c}
    to_x = {"fsdp": fx}
    to_y = {"row": 1 - row}
    to_z = {"dp": 1 - dp}
    to_xy = {"row": row + (1 - c) * (1 - 2 * row), "fsdp": f + c * (fx - f)}
    to_first = {"row": row + c * (1 - 2 * row), "fsdp": f + (1 - c) * (fx - f)}

    out_l, mid_l = 64 * c, 128 * (1 - c)

    def w_load(n):
        i, mid = n // 2, n % 2
        src = (w1_hbm, w3_hbm, w2_hbm)[i]
        if mid:
            return pltpu.make_async_copy(
                src.at[pl.ds(pl.multiple_of(mid_l, 64), 64), :], w.at[i, pl.ds(pl.multiple_of(OWN_MID + 64 * c, 64), 64), :], wl_sem.at[n]
            )
        return pltpu.make_async_copy(
            src.at[pl.ds(pl.multiple_of(out_l, 64), 128), :], w.at[i, pl.ds(pl.multiple_of(OWN_OUT + 128 * c, 128), 128), :], wl_sem.at[n]
        )

    def g_load(k, side):
        half = 1 - dp if k < 3 else dp
        core = c if side == 0 else 1 - c
        rows = pl.ds(pl.multiple_of(864 * core + 432 * half + CH * (k % 3), 16), CH)
        slot = 2 * (k % 3) + side
        return pltpu.make_async_copy(g_hbm.at[rows, :], stage.at[slot], st_sem.at[slot])

    def t_load(t, which):
        src, dst = ((x_hbm, xv), (dy_hbm, dv))[which]
        cols = pl.ds(t * 1024, 1024)
        return pltpu.make_async_copy(src.at[:, cols], dst.at[:, cols], in_sem.at[2 * t + which])

    for n in (0, 2, 4, 1, 3, 5):
        w_load(n).start()
    for k in range(3):
        g_load(k, 1).start()
        g_load(k, 0).start()
        if k == 0:
            t_load(0, 0).start()
            t_load(0, 1).start()
    for t in range(1, TA // 1024):
        t_load(t, 0).start()
        t_load(t, 1).start()

    barrier = pltpu.get_barrier_semaphore()
    for peer in (to_core, to_x, to_y, to_z):
        pl.semaphore_signal(barrier, inc=1, device_id=peer, device_id_type=MESH)
    pl.semaphore_wait(barrier, 4)

    def w_rows(base, size):
        return w.at[:, pl.ds(pl.multiple_of(base, 64), size), :]

    def w_copy(n):
        o, m = 128 * c, 64 * c
        src, dst, size, peer = (
            (OWN_OUT + o, OWN_OUT + o, 128, to_core),
            (OWN_OUT + o, X_OUT + o, 128, to_x),
            (OWN_OUT + o, Y_OUT + o, 128, to_y),
            (OWN_MID + m, OWN_MID + m, 64, to_core),
            (OWN_MID + m, X_MID + m, 64, to_x),
            (OWN_MID + m, Y_MID + m, 64, to_y),
            (X_OUT + o, X_OUT + o, 128, to_core),
            (Y_OUT + o, Y_OUT + o, 128, to_core),
            (X_MID + m, X_MID + m, 64, to_core),
            (Y_MID + m, Y_MID + m, 64, to_core),
            (X_OUT + c * (Y_OUT + 128 - X_OUT), DIAG + 256 * c, 128, to_xy),
            (X_MID + c * (Y_MID + 64 - X_MID), DIAG + 128 + m, 64, to_xy),
            (DIAG + 256 * c, DIAG + 256 * c, 128, to_core),
            (DIAG + 128 + m, DIAG + 128 + m, 64, to_core),
        )[n]
        return pltpu.make_async_remote_copy(
            src_ref=w_rows(src, size), dst_ref=w_rows(dst, size), send_sem=ws.at[n], recv_sem=wr.at[n], device_id=peer, device_id_type=MESH
        )

    def w_send(*ns):
        for n in ns:
            w_copy(n).start()

    def w_arrived(*ns):
        for n in ns:
            w_copy(n).wait_recv()

    def remote(src, dst, s, r, peer):
        return pltpu.make_async_remote_copy(src_ref=src, dst_ref=dst, send_sem=s, recv_sem=r, device_id=peer, device_id_type=MESH)

    def p_copy(k):
        return remote(part.at[k], r0.at[k], p_s.at[k], p_r.at[k], to_core)

    def z_copy(k):
        return remote(acc.at[k], rz.at[k], z_s.at[k], z_r.at[k], to_z)

    def cols(q):
        return pl.ds(pl.multiple_of(q * BLK, BLK), BLK)

    def q_of(j, mine):
        on_x = 2 * j + (x if mine else 1 - x)
        on_y = 2 * (row if mine else 1 - row) + j
        return (1 - c) * on_x + c * on_y

    def d1_copy(k, j):
        return remote(acc.at[3 + k, :, cols(q_of(j, False))], r1.at[k, :, pl.ds(BLK * j, BLK)], d1_s.at[k, j], d1_r.at[k, j], to_first)

    m = (1 - c) * row + c * x

    def d2_copy(k):
        return remote(kept.at[k, :, cols(1 - m)], r2.at[k], d2_s.at[k], d2_r.at[k], to_xy)

    def za_copy(k):
        return remote(own.at[3 * dp + k], own.at[3 * dp + k], za_s.at[k], za_r.at[k], to_z)

    def za_arrival(k):
        return remote(own.at[3 * dp + k], own.at[3 * (1 - dp) + k], za_s.at[k], za_r.at[k], to_z)

    def lanes(core):
        return pl.ds(pl.multiple_of(128 * core, 128), 256)

    f_copy = remote(own.at[:, :, lanes(1 - c)], theirs, f_s, f_r, to_core)
    own_out = pltpu.make_async_copy(own.at[:, :, lanes(c)], sum_out.at[pl.ds(6 * c, 6)], out_sem.at[0])
    their_out = pltpu.make_async_copy(theirs, sum_out.at[pl.ds(6 * (1 - c), 6)], out_sem.at[1])
    w_store = pltpu.make_async_copy(w, w_out, out_sem.at[2])

    def convert(base):
        for k in range(base, base + 3):
            g_load(k, 1).wait()
            part[k] = stage[2 * (k - base) + 1].astype(BF)
            g_load(k, 0).wait()
            acc[k] = stage[2 * (k - base)].astype(BF)
            if k > base:
                p_copy(k - 1).start()
        p_copy(base + 2).start()

    def add_partner(base):
        for k in range(base, base + 3):
            p_copy(k).wait_recv()
            acc[k] = acc[k] + r0[k]

    def z_step(k):
        z_copy(k).wait_recv()
        acc[3 + k] = acc[3 + k] + rz[k]
        d1_copy(k, 0).start()
        d1_copy(k, 1).start()

    def d1_step(k):
        for j in range(2):
            d1_copy(k, j).wait_recv()
        for j in range(2):
            at = pl.ds(BLK * j, BLK)
            kept[k, :, at] = acc[3 + k, :, cols(q_of(j, True))] + r1[k, :, at]
        d2_copy(k).start()

    def d2_step(k):
        d2_copy(k).wait_recv()
        own[3 * dp + k] = kept[k, :, cols(m)] + r2[k]
        za_copy(k).start()

    def dw_copy(slot, i, base):
        return pltpu.make_async_copy(dwo.at[slot], dw_out.at[i, :, pl.ds(pl.multiple_of(base, 256), 256)], dwo_sem.at[slot])

    def dx_copy(t, size):
        at = pl.ds(pl.multiple_of(t * size, size), size)
        return pltpu.make_async_copy(dxo.at[lax.rem(t, 2)], dx_out.at[:, at], dxo_sem.at[lax.rem(t, 2)])

    def f_tile(base, size, t, tile, first, last):
        rows = pl.ds(base, size)
        at = pl.ds(pl.multiple_of(t * tile, tile), tile)
        h, da, db = forward_tile(xv[:, at], dv[:, at], w, rows)
        h_s[:size, at] = h
        da_s[:size, at] = da
        db_s[:size, at] = db
        dx = dx_tile(da, db, w, rows)
        if first:
            dxa[:, at] = dx
        elif last:

            @pl.when(t >= 2)
            def _():
                dx_copy(t - 2, tile).wait()

            dxo[lax.rem(t, 2)] = (dxa[:, at] + dx).astype(BF)
            dx_copy(t, tile).start()
        else:
            dxa[:, at] += dx

    def w_chunk(base, n, i, fresh):
        if not fresh:
            dw_copy(i, i, base + 256 * n - 256).wait()
        at = pl.ds(pl.multiple_of(256 * n, 256), 256)
        lhs = (xv, xv, dv)[i]
        rhs = (da_s, db_s, h_s)[i]
        dwo[i] = dot(lhs[...], rhs[at, :], NT)
        dw_copy(i, i, base + 256 * n).start()

    for n in (0, 2, 4):
        w_load(n).wait()
    w_send(0, 1, 2)
    for n in (1, 3, 5):
        w_load(n).wait()
    w_send(3, 4, 5)
    convert(0)
    for k in range(3, 6):
        g_load(k, 1).start()
        g_load(k, 0).start()
    w_arrived(0)

    @pl.loop(0, TA // 1024)
    def _(t):
        for i in range(TA // 1024):

            @pl.when(t == i)
            def _():
                t_load(i, 0).wait()
                t_load(i, 1).wait()

        @pl.when(t == 1)
        def _():
            convert(3)
            add_partner(0)
            for k in range(3):
                z_copy(k).start()

        f_tile(0, 256, t, 1024, True, False)

    add_partner(3)
    w_chunk(0, 0, 0, True)
    w_chunk(0, 0, 1, True)
    w_arrived(1, 2)
    w_send(6, 7, 10)
    w_chunk(0, 0, 2, True)
    w_arrived(6, 7)

    @pl.loop(0, TA // 1024)
    def _(t):
        @pl.when(t == 2)
        def _():
            w_arrived(3, 4, 5)
            w_send(8, 9, 11)
            z_step(0)

        f_tile(256, 512, t, 1024, False, False)

    d1_step(0)
    for i in range(3):
        dw_copy(i, i, 0).wait()

    @pl.loop(0, 2)
    def _(n):
        @pl.when(n == 1)
        def _():
            d2_step(0)
            w_arrived(10, 11)
            w_send(12, 13)

        for i in range(3):

            @pl.when(n > 0)
            def _():
                dw_copy(i, i, 256 + 256 * n - 256).wait()

            w_chunk(256, n, i, True)

    w_arrived(8, 9, 12, 13)
    w_store.start()
    z_step(1)
    for i in range(3):
        dw_copy(i, i, 512).wait()

    @pl.loop(0, TA // 512)
    def _(t):
        for i, step in enumerate((None, lambda: d1_step(1), lambda: d2_step(1), lambda: z_step(2), lambda: d1_step(2), lambda: d2_step(2))):
            if step is not None:
                pl.when(t == i)(step)
        f_tile(768, 768, t, 512, False, True)

    for k in range(3):
        za_arrival(k).wait_recv()
    f_copy.start()
    own_out.start()

    @pl.loop(0, 3)
    def _(n):
        @pl.when(n == 2)
        def _():
            f_copy.wait_recv()
            their_out.start()

        for i in range(3):

            @pl.when(n > 0)
            def _():
                dw_copy(i, i, 768 + 256 * n - 256).wait()

            w_chunk(768, n, i, True)

    for i in range(3):
        dw_copy(i, i, 1280).wait()
    for t in (TA // 512 - 2, TA // 512 - 1):
        dx_copy(t, 512).wait()
    own_out.wait()
    their_out.wait()
    w_store.wait()
    for n in range(14):
        w_copy(n).wait_send()
    for k in range(6):
        p_copy(k).wait_send()
    for k in range(3):
        z_copy(k).wait_send()
        d1_copy(k, 0).wait_send()
        d1_copy(k, 1).wait_send()
        d2_copy(k).wait_send()
        za_copy(k).wait_send()
    f_copy.wait_send()


def kernel_b(
    x_hbm, dy_hbm, w_hbm, dwp_hbm, dxp_hbm, sum_hbm,
    dx_out, dw_out, dn_out,
    xv, dv, w, dwp, dxp, sums, flip, dn, da_s, db_s, h_s, dxa, dxo, dwo,
    t_sem, w_sem, dwp_sem, misc_sem, dwo_sem, out_sem,
):
    row = lax.axis_index("row")
    f = lax.axis_index("fsdp")
    c = lax.rem(f, 2)
    x = f // 2
    q_own, q_x, q_y, q_d = 2 * row + x, 2 * row + 1 - x, 2 * (1 - row) + x, 2 * (1 - row) + 1 - x
    granule = [3 * q + j for q, j in (
        (q_own, 0), (q_own, 2), (q_x, 0), (q_x, 2), (q_y, 0), (q_y, 2), (q_own, 1), (q_x, 1), (q_y, 1), (q_d, 0), (q_d, 1), (q_d, 2)
    )]

    def t_load(t, which):
        src, dst = ((x_hbm, xv), (dy_hbm, dv))[which]
        return pltpu.make_async_copy(src.at[:, pl.ds(TA + 512 * t, 512)], dst.at[:, pl.ds(512 * t, 512)], t_sem.at[2 * t + which])

    def w_load(g, i):
        rows = pl.ds(768 * g, 768)
        return pltpu.make_async_copy(w_hbm.at[i, rows, :], w.at[i, rows, :], w_sem.at[3 * g + i])

    def dwp_load(g):
        at = pl.ds(768 * g, 768)
        return pltpu.make_async_copy(dwp_hbm.at[:, :, at], dwp.at[:, :, at], dwp_sem.at[g])

    sum_load = pltpu.make_async_copy(sum_hbm, sums, misc_sem.at[0])
    dxp_load = pltpu.make_async_copy(dxp_hbm, dxp, misc_sem.at[1])
    dxp_store = pltpu.make_async_copy(dxp, dx_out.at[:, pl.ds(0, TA)], misc_sem.at[2])
    dx_store = pltpu.make_async_copy(dxo, dx_out.at[:, pl.ds(TA, TB)], out_sem.at[0])
    dn_store = pltpu.make_async_copy(dn, dn_out, out_sem.at[1])

    w_load(0, 0).start()
    t_load(0, 0).start()
    w_load(0, 1).start()
    w_load(0, 2).start()
    t_load(0, 1).start()
    t_load(1, 0).start()
    t_load(1, 1).start()
    sum_load.start()
    dwp_load(0).start()
    for i in range(3):
        w_load(1, i).start()
    dxp_load.start()
    dwp_load(1).start()
    for i in range(3):
        w_load(0, i).wait()

    def dw_copy(g, n, i, part, slot):
        k = 6 * g + part
        where = granule[k]
        for j in (1, 2):
            where = where + jnp.where(n == j, granule[k + 2 * j] - granule[k], 0)
        return pltpu.make_async_copy(
            dwo.at[slot, :, pl.ds(128 * part, 128)], dw_out.at[i, :, pl.ds(pl.multiple_of(128 * where, 128), 128)], dwo_sem.at[slot, part]
        )

    for g in range(2):
        rows = pl.ds(768 * g, 768)
        if g == 1:
            for i in range(3):
                w_load(1, i).wait()

        @pl.loop(0, TB // 512)
        def _(t):
            if g == 0:
                for i in range(TB // 512):

                    @pl.when(t == i)
                    def _():
                        t_load(i, 0).wait()
                        t_load(i, 1).wait()

            at = pl.ds(pl.multiple_of(t * 512, 512), 512)
            h, da, db = forward_tile(xv[:, at], dv[:, at], w, rows)
            h_s[:, at] = h
            da_s[:, at] = da
            db_s[:, at] = db
            dx = dx_tile(da, db, w, rows)
            if g == 0:
                dxa[:, at] = dx
            else:
                dxo[:, at] = (dxa[:, at] + dx).astype(BF)

        if g == 0:
            sum_load.wait()
            for i in range(3):
                flip[...] = jnp.transpose(sums[pl.ds(576 * i, 576), :].astype(F32))
                dn[i] = flip[pl.ds(pl.multiple_of(64 * c, 64), 192), :]
            dn_store.start()
        else:
            dx_store.start()
            dxp_load.wait()
            dxp_store.start()
        dwp_load(g).wait()

        @pl.loop(0, 3)
        def _(n):
            for i in range(3):
                for part in range(2):

                    @pl.when(n > 0)
                    def _():
                        dw_copy(g, n - 1, i, part, i).wait()

                    if g == 1:

                        @pl.when(n == 0)
                        def _():
                            dw_copy(0, 2, i, part, i).wait()

                cut = pl.ds(pl.multiple_of(256 * n, 256), 256)
                at = pl.ds(pl.multiple_of(768 * g + 256 * n, 256), 256)
                lhs = (xv, xv, dv)[i]
                rhs = (da_s, db_s, h_s)[i]
                dwo[i] = dwp[i, :, at] + dot(lhs[...], rhs[cut, :], NT)
                for part in range(2):
                    dw_copy(g, n, i, part, i).start()

    for i in range(3):
        for part in range(2):
            dw_copy(1, 2, i, part, i).wait()
    dx_store.wait()
    dxp_store.wait()
    dn_store.wait()


def per_device(x_blk, dy_blk, gate_shard, up_shard, down_shard, g_part):
    x_t, dy_t = x_blk.T, dy_blk.T
    dma = pltpu.SemaphoreType.DMA
    vm = pltpu.VMEM
    shape = jax.ShapeDtypeStruct
    w_all, dw_part, dx_part, sums = pl.pallas_call(
        kernel_a,
        out_shape=(shape((3, H, D), BF), shape((3, D, H), F32), shape((D, TA), BF), shape((12, CH, 256), BF)),
        in_specs=[ANY] * 6,
        out_specs=(ANY,) * 4,
        scratch_shapes=[
            vm((D, TA), BF), vm((D, TA), BF), vm((3, H, D), BF), vm((768, TA), BF), vm((768, TA), BF), vm((768, TA), BF),
            vm((D, TA), F32), vm((2, D, 512), BF), vm((3, D, 256), F32),
            vm((6, CH, H), F32), vm((6, CH, H), BF), vm((6, CH, H), BF), vm((6, CH, H), BF), vm((3, CH, H), BF),
            vm((3, CH, 2 * BLK), BF), vm((3, CH, 2 * BLK), BF), vm((3, CH, BLK), BF), vm((6, CH, BLK), BF), vm((6, CH, 256), BF),
            dma((TA // 512,)), dma((6,)), dma((14,)), dma((14,)), dma((6,)), dma((6,)), dma((6,)), dma((3,)), dma((3,)),
            dma((3, 2)), dma((3, 2)), dma((3,)), dma((3,)), dma((3,)), dma((3,)), dma, dma, dma((2,)), dma((3,)), dma((3,)),
        ],
        compiler_params=pltpu.CompilerParams(collective_id=0, has_side_effects=True, vmem_limit_bytes=VMEM_LIMIT),
        name="gather_reduce_backward",
    )(x_t, dy_t, gate_shard.T, up_shard.T, down_shard, g_part.reshape(3 * D, H))
    dx_t, dw_local, dn_t = pl.pallas_call(
        kernel_b,
        out_shape=(shape((D, T), BF), shape((3, D, H), F32), shape((3, 192, D), F32)),
        in_specs=[ANY] * 6,
        out_specs=(ANY,) * 3,
        scratch_shapes=[
            vm((D, TB), BF), vm((D, TB), BF), vm((3, H, D), BF), vm((3, D, H), F32), vm((D, TA), BF), vm((3 * D, 256), BF),
            vm((256, D), F32), vm((3, 192, D), F32), vm((768, TB), BF), vm((768, TB), BF), vm((768, TB), BF),
            vm((D, TB), F32), vm((D, TB), BF), vm((3, D, 256), F32),
            dma((TB // 256,)), dma((6,)), dma((2,)), dma((3,)), dma((3, 2)), dma((2,)),
        ],
        compiler_params=pltpu.CompilerParams(vmem_limit_bytes=VMEM_LIMIT),
        name="finish_backward",
    )(x_t, dy_t, w_all, dw_part, dx_part, sums.reshape(3 * D, 256))
    return dx_t.T, jnp.swapaxes(dn_t, 1, 2), dw_local[None]


def solution(mesh):
    return jax.shard_map(
        per_device,
        mesh=mesh,
        in_specs=(P(ALL_AXES, None), P(ALL_AXES, None), P(None, GROUP_AXES), P(None, GROUP_AXES), P(GROUP_AXES, None), P(ALL_AXES, None, None, None)),
        out_specs=(P(ALL_AXES, None), P(None, None, GROUP_AXES), P(ALL_AXES, None, None, None)),
        check_vma=False,
    )
```

```python
import jax
import jax.numpy as jnp
from jax import lax
from jax.experimental import pallas as pl
from jax.experimental.pallas import tpu as pltpu
from jax.sharding import PartitionSpec as P

ALL_AXES = ("dp", "row", "fsdp")
GROUP_AXES = ("row", "fsdp")
MESH = pl.DeviceIdType.MESH
NN = (((1,), (0,)), ((), ()))
NT = (((1,), (1,)), ((), ()))
TN = (((0,), (0,)), ((), ()))
F32 = jnp.float32
BF = jnp.bfloat16
ANY = pl.BlockSpec(memory_space=pl.ANY)

D = 576
H = 1536
T = 4096
TA = 3072
TB = T - TA
CH = 144
BLK = 384
VMEM_LIMIT = 67043328
OWN_OUT, X_OUT, Y_OUT, OWN_MID, X_MID, Y_MID, DIAG = 0, 256, 512, 768, 896, 1024, 1152


def dot(lhs, rhs, dims):
    return lax.dot_general(lhs, rhs, dims, preferred_element_type=F32)


def forward_tile(x, dy, w, rows):
    a = dot(w[0, rows, :], x, NN)
    b = dot(w[1, rows, :], x, NN)
    dh = dot(w[2, rows, :], dy, NN)
    s = jax.nn.sigmoid(a)
    silu = a * s
    h = (silu * b).astype(BF)
    da = (dh * b * s * (1.0 + a * (1.0 - s))).astype(BF)
    db = (dh * silu).astype(BF)
    return h, da, db


def dx_tile(da, db, w, rows):
    return dot(w[0, rows, :], da, TN) + dot(w[1, rows, :], db, TN)


def kernel_a(
    x_hbm, dy_hbm, w1_hbm, w3_hbm, w2_hbm, g_hbm,
    w_out, dw_out, dx_out, sum_out,
    xv, dv, w, da_s, db_s, h_s, dxa, dxo, dwa,
    stage, part, r0, acc, rz, r1, kept, r2, own, theirs,
    in_sem, wl_sem, ws, wr, st_sem, p_s, p_r, z_s, z_r, d1_s, d1_r, d2_s, d2_r, za_s, za_r, f_s, f_r, dxo_sem, dwo_sem, out_sem,
):
    dp = lax.axis_index("dp")
    row = lax.axis_index("row")
    f = lax.axis_index("fsdp")
    c = lax.rem(f, 2)
    x = f // 2
    fx = lax.rem(f + 2, 4)
    to_core = {"fsdp": f + 1 - 2 * c}
    to_x = {"fsdp": fx}
    to_y = {"row": 1 - row}
    to_z = {"dp": 1 - dp}
    to_xy = {"row": row + (1 - c) * (1 - 2 * row), "fsdp": f + c * (fx - f)}
    to_first = {"row": row + c * (1 - 2 * row), "fsdp": f + (1 - c) * (fx - f)}

    out_l, mid_l = 64 * c, 128 * (1 - c)

    def w_load(n):
        i, mid = n // 2, n % 2
        src = (w1_hbm, w3_hbm, w2_hbm)[i]
        if mid:
            return pltpu.make_async_copy(
                src.at[pl.ds(pl.multiple_of(mid_l, 64), 64), :], w.at[i, pl.ds(pl.multiple_of(OWN_MID + 64 * c, 64), 64), :], wl_sem.at[n]
            )
        return pltpu.make_async_copy(
            src.at[pl.ds(pl.multiple_of(out_l, 64), 128), :], w.at[i, pl.ds(pl.multiple_of(OWN_OUT + 128 * c, 128), 128), :], wl_sem.at[n]
        )

    def g_load(k, side):
        half = 1 - dp if k < 3 else dp
        core = c if side == 0 else 1 - c
        rows = pl.ds(pl.multiple_of(864 * core + 432 * half + CH * (k % 3), 16), CH)
        slot = 2 * (k % 3) + side
        return pltpu.make_async_copy(g_hbm.at[rows, :], stage.at[slot], st_sem.at[slot])

    def t_load(t, which):
        src, dst = ((x_hbm, xv), (dy_hbm, dv))[which]
        cols = pl.ds(t * 1024, 1024)
        return pltpu.make_async_copy(src.at[:, cols], dst.at[:, cols], in_sem.at[2 * t + which])

    for n in (0, 2, 4, 1, 3, 5):
        w_load(n).start()
    for k in range(3):
        g_load(k, 1).start()
        g_load(k, 0).start()
        if k == 0:
            t_load(0, 0).start()
            t_load(0, 1).start()
    for t in range(1, TA // 1024):
        t_load(t, 0).start()
        t_load(t, 1).start()

    barrier = pltpu.get_barrier_semaphore()
    for peer in (to_core, to_x, to_y, to_z):
        pl.semaphore_signal(barrier, inc=1, device_id=peer, device_id_type=MESH)
    for i in range(3):
        dwa[i] = jnp.zeros((D, H), F32)
    pl.semaphore_wait(barrier, 4)

    def w_rows(base, size):
        return w.at[:, pl.ds(pl.multiple_of(base, 64), size), :]

    def w_copy(n):
        o, m = 128 * c, 64 * c
        src, dst, size, peer = (
            (OWN_OUT + o, OWN_OUT + o, 128, to_core),
            (OWN_OUT + o, X_OUT + o, 128, to_x),
            (OWN_OUT + o, Y_OUT + o, 128, to_y),
            (OWN_MID + m, OWN_MID + m, 64, to_core),
            (OWN_MID + m, X_MID + m, 64, to_x),
            (OWN_MID + m, Y_MID + m, 64, to_y),
            (X_OUT + o, X_OUT + o, 128, to_core),
            (Y_OUT + o, Y_OUT + o, 128, to_core),
            (X_MID + m, X_MID + m, 64, to_core),
            (Y_MID + m, Y_MID + m, 64, to_core),
            (X_OUT + c * (Y_OUT + 128 - X_OUT), DIAG + 256 * c, 128, to_xy),
            (X_MID + c * (Y_MID + 64 - X_MID), DIAG + 128 + m, 64, to_xy),
            (DIAG + 256 * c, DIAG + 256 * c, 128, to_core),
            (DIAG + 128 + m, DIAG + 128 + m, 64, to_core),
        )[n]
        return pltpu.make_async_remote_copy(
            src_ref=w_rows(src, size), dst_ref=w_rows(dst, size), send_sem=ws.at[n], recv_sem=wr.at[n], device_id=peer, device_id_type=MESH
        )

    def w_send(*ns):
        for n in ns:
            w_copy(n).start()

    def w_arrived(*ns):
        for n in ns:
            w_copy(n).wait_recv()

    def remote(src, dst, s, r, peer):
        return pltpu.make_async_remote_copy(src_ref=src, dst_ref=dst, send_sem=s, recv_sem=r, device_id=peer, device_id_type=MESH)

    def p_copy(k):
        return remote(part.at[k], r0.at[k], p_s.at[k], p_r.at[k], to_core)

    def z_copy(k):
        return remote(acc.at[k], rz.at[k], z_s.at[k], z_r.at[k], to_z)

    def cols(q):
        return pl.ds(pl.multiple_of(q * BLK, BLK), BLK)

    def q_of(j, mine):
        on_x = 2 * j + (x if mine else 1 - x)
        on_y = 2 * (row if mine else 1 - row) + j
        return (1 - c) * on_x + c * on_y

    def d1_copy(k, j):
        return remote(acc.at[3 + k, :, cols(q_of(j, False))], r1.at[k, :, pl.ds(BLK * j, BLK)], d1_s.at[k, j], d1_r.at[k, j], to_first)

    m = (1 - c) * row + c * x

    def d2_copy(k):
        return remote(kept.at[k, :, cols(1 - m)], r2.at[k], d2_s.at[k], d2_r.at[k], to_xy)

    def za_copy(k):
        return remote(own.at[3 * dp + k], own.at[3 * dp + k], za_s.at[k], za_r.at[k], to_z)

    def za_arrival(k):
        return remote(own.at[3 * dp + k], own.at[3 * (1 - dp) + k], za_s.at[k], za_r.at[k], to_z)

    def lanes(core):
        return pl.ds(pl.multiple_of(128 * core, 128), 256)

    f_copy = remote(own.at[:, :, lanes(1 - c)], theirs, f_s, f_r, to_core)
    own_out = pltpu.make_async_copy(own.at[:, :, lanes(c)], sum_out.at[pl.ds(6 * c, 6)], out_sem.at[0])
    their_out = pltpu.make_async_copy(theirs, sum_out.at[pl.ds(6 * (1 - c), 6)], out_sem.at[1])
    w_store = pltpu.make_async_copy(w, w_out, out_sem.at[2])

    def convert(base):
        for k in range(base, base + 3):
            g_load(k, 1).wait()
            part[k] = stage[2 * (k - base) + 1].astype(BF)
            g_load(k, 0).wait()
            acc[k] = stage[2 * (k - base)].astype(BF)
            if k > base:
                p_copy(k - 1).start()
        p_copy(base + 2).start()

    def add_partner(base):
        for k in range(base, base + 3):
            p_copy(k).wait_recv()
            acc[k] = acc[k] + r0[k]

    def z_step(k):
        z_copy(k).wait_recv()
        acc[3 + k] = acc[3 + k] + rz[k]
        d1_copy(k, 0).start()
        d1_copy(k, 1).start()

    def d1_step(k):
        for j in range(2):
            d1_copy(k, j).wait_recv()
        for j in range(2):
            at = pl.ds(BLK * j, BLK)
            kept[k, :, at] = acc[3 + k, :, cols(q_of(j, True))] + r1[k, :, at]
        d2_copy(k).start()

    def d2_step(k):
        d2_copy(k).wait_recv()
        own[3 * dp + k] = kept[k, :, cols(m)] + r2[k]
        za_copy(k).start()

    def dw_copy(n, base, size):
        at = pl.ds(base, size)
        return pltpu.make_async_copy(dwa.at[:, :, at], dw_out.at[:, :, at], dwo_sem.at[n])

    def dx_copy(t, size):
        at = pl.ds(pl.multiple_of(t * size, size), size)
        return pltpu.make_async_copy(dxo.at[lax.rem(t, 2)], dx_out.at[:, at], dxo_sem.at[lax.rem(t, 2)])

    def tile_step(base, size, t, tile, first, last):
        rows = pl.ds(base, size)
        at = pl.ds(pl.multiple_of(t * tile, tile), tile)
        xt, dyt = xv[:, at], dv[:, at]
        h_s[:size, :tile], da_s[:size, :tile], db_s[:size, :tile] = forward_tile(xt, dyt, w, rows)
        h, da, db = h_s[:size, :tile], da_s[:size, :tile], db_s[:size, :tile]
        dx = dx_tile(da, db, w, rows)
        if first:
            dxa[:, at] = dx
        elif last:
            dxo[lax.rem(t, 2)] = (dxa[:, at] + dx).astype(BF)
        else:
            dxa[:, at] += dx
        dwa[0, :, rows] += dot(xt, da, NT)
        dwa[1, :, rows] += dot(xt, db, NT)
        dwa[2, :, rows] += dot(dyt, h, NT)

    for n in (0, 2, 4):
        w_load(n).wait()
    w_send(0, 1, 2)
    for n in (1, 3, 5):
        w_load(n).wait()
    w_send(3, 4, 5)
    convert(0)
    for k in range(3, 6):
        g_load(k, 1).start()
        g_load(k, 0).start()
    w_arrived(0)

    @pl.loop(0, TA // 1024)
    def _(t):
        for i in range(TA // 1024):

            @pl.when(t == i)
            def _():
                t_load(i, 0).wait()
                t_load(i, 1).wait()

        @pl.when(t == 1)
        def _():
            convert(3)
            add_partner(0)
            for k in range(3):
                z_copy(k).start()

        tile_step(0, 256, t, 1024, True, False)

    dw_copy(0, 0, 256).start()
    w_arrived(1, 2)
    w_send(6, 7, 10)
    add_partner(3)
    w_arrived(6, 7)

    @pl.loop(0, TA // 1024)
    def _(t):
        @pl.when(t == 1)
        def _():
            w_arrived(3, 4, 5)
            w_send(8, 9, 11)
            z_step(0)

        @pl.when(t == 2)
        def _():
            w_arrived(10, 11)
            w_send(12, 13)
            d1_step(0)

        tile_step(256, 512, t, 1024, False, False)

    dw_copy(1, 256, 512).start()
    d2_step(0)
    w_arrived(8, 9, 12, 13)
    w_store.start()

    def g_output():
        for k in range(3):
            za_arrival(k).wait_recv()
        f_copy.start()
        own_out.start()

    def z2_d21():
        z_step(2)
        d2_step(1)

    @pl.loop(0, TA // 512)
    def _(t):
        steps = (lambda: z_step(1), lambda: d1_step(1), z2_d21, lambda: d1_step(2), lambda: d2_step(2), g_output)
        for i, step in enumerate(steps):
            pl.when(t == i)(step)

        @pl.when(t >= 2)
        def _():
            dx_copy(t - 2, 512).wait()

        tile_step(768, 768, t, 512, False, True)
        dx_copy(t, 512).start()

    dw_copy(2, 768, 768).start()
    f_copy.wait_recv()
    their_out.start()
    for t in (TA // 512 - 2, TA // 512 - 1):
        dx_copy(t, 512).wait()
    own_out.wait()
    their_out.wait()
    w_store.wait()
    for n in range(14):
        w_copy(n).wait_send()
    for k in range(6):
        p_copy(k).wait_send()
    for k in range(3):
        z_copy(k).wait_send()
        d1_copy(k, 0).wait_send()
        d1_copy(k, 1).wait_send()
        d2_copy(k).wait_send()
        za_copy(k).wait_send()
    f_copy.wait_send()
    dw_copy(0, 0, 256).wait()
    dw_copy(1, 256, 512).wait()
    dw_copy(2, 768, 768).wait()


def kernel_b(
    x_hbm, dy_hbm, w_hbm, dwp_hbm, dxp_hbm, sum_hbm,
    dx_out, dw_out, dn_out,
    xv, dv, w, dwa, dxp, sums, flip, dn, da_s, db_s, h_s, dxa, dxo,
    t_sem, w_sem, dwp_sem, misc_sem, dwo_sem, out_sem,
):
    row = lax.axis_index("row")
    f = lax.axis_index("fsdp")
    c = lax.rem(f, 2)
    x = f // 2
    q_own, q_x, q_y, q_d = 2 * row + x, 2 * row + 1 - x, 2 * (1 - row) + x, 2 * (1 - row) + 1 - x
    granule = [3 * q + j for q, j in (
        (q_own, 0), (q_own, 2), (q_x, 0), (q_x, 2), (q_y, 0), (q_y, 2), (q_own, 1), (q_x, 1), (q_y, 1), (q_d, 0), (q_d, 1), (q_d, 2)
    )]

    def t_load(t, which):
        src, dst = ((x_hbm, xv), (dy_hbm, dv))[which]
        return pltpu.make_async_copy(src.at[:, pl.ds(TA + 512 * t, 512)], dst.at[:, pl.ds(512 * t, 512)], t_sem.at[2 * t + which])

    def w_load(g, i):
        rows = pl.ds(768 * g, 768)
        return pltpu.make_async_copy(w_hbm.at[i, rows, :], w.at[i, rows, :], w_sem.at[3 * g + i])

    def dwp_load(g):
        at = pl.ds(768 * g, 768)
        return pltpu.make_async_copy(dwp_hbm.at[:, :, at], dwa.at[:, :, at], dwp_sem.at[g])

    sum_load = pltpu.make_async_copy(sum_hbm, sums, misc_sem.at[0])
    dxp_load = pltpu.make_async_copy(dxp_hbm, dxp, misc_sem.at[1])
    dxp_store = pltpu.make_async_copy(dxp, dx_out.at[:, pl.ds(0, TA)], misc_sem.at[2])
    dx_store = pltpu.make_async_copy(dxo, dx_out.at[:, pl.ds(TA, TB)], out_sem.at[0])
    dn_store = pltpu.make_async_copy(dn, dn_out, out_sem.at[1])

    w_load(0, 0).start()
    t_load(0, 0).start()
    w_load(0, 1).start()
    w_load(0, 2).start()
    t_load(0, 1).start()
    t_load(1, 0).start()
    t_load(1, 1).start()
    sum_load.start()
    dwp_load(0).start()
    for i in range(3):
        w_load(1, i).start()
    dxp_load.start()
    dwp_load(1).start()
    for i in range(3):
        w_load(0, i).wait()

    def dw_copy(k):
        at = pl.ds(pl.multiple_of(128 * granule[k], 128), 128)
        return pltpu.make_async_copy(dwa.at[:, :, pl.ds(128 * k, 128)], dw_out.at[:, :, at], dwo_sem.at[k])

    def tile_step(g, t, between):
        rows = pl.ds(768 * g, 768)
        at = pl.ds(pl.multiple_of(t * 512, 512), 512)
        xt, dyt = xv[:, at], dv[:, at]
        h_s[...], da_s[...], db_s[...] = forward_tile(xt, dyt, w, rows)
        h, da, db = h_s[...], da_s[...], db_s[...]
        dx = dx_tile(da, db, w, rows)
        if g == 0:
            dxa[:, at] = dx
        else:
            dxo[:, at] = (dxa[:, at] + dx).astype(BF)
        if between is not None:
            between()
        dwa[0, :, rows] += dot(xt, da, NT)
        dwa[1, :, rows] += dot(xt, db, NT)
        dwa[2, :, rows] += dot(dyt, h, NT)

    for t in range(2):
        for which in range(2):
            t_load(t, which).wait()
        tile_step(0, t, dwp_load(0).wait if t == 0 else None)
    for k in range(6):
        dw_copy(k).start()
    sum_load.wait()
    for i in range(3):
        flip[...] = jnp.transpose(sums[pl.ds(576 * i, 576), :].astype(F32))
        dn[i] = flip[pl.ds(pl.multiple_of(64 * c, 64), 192), :]
    dn_store.start()
    for i in range(3):
        w_load(1, i).wait()
    dxp_load.wait()
    dxp_store.start()
    dwp_load(1).wait()

    @pl.loop(0, TB // 512)
    def _(t):
        tile_step(1, t, None)

    for k in range(6, 12):
        dw_copy(k).start()
    dx_store.start()
    for k in range(12):
        dw_copy(k).wait()
    dx_store.wait()
    dxp_store.wait()
    dn_store.wait()


def per_device(x_blk, dy_blk, gate_shard, up_shard, down_shard, g_part):
    x_t, dy_t = x_blk.T, dy_blk.T
    dma = pltpu.SemaphoreType.DMA
    vm = pltpu.VMEM
    shape = jax.ShapeDtypeStruct
    w_all, dw_part, dx_part, sums = pl.pallas_call(
        kernel_a,
        out_shape=(shape((3, H, D), BF), shape((3, D, H), F32), shape((D, TA), BF), shape((12, CH, 256), BF)),
        in_specs=[ANY] * 6,
        out_specs=(ANY,) * 4,
        scratch_shapes=[
            vm((D, TA), BF), vm((D, TA), BF), vm((3, H, D), BF), vm((768, 1024), BF), vm((768, 1024), BF), vm((768, 1024), BF),
            vm((D, TA), F32), vm((2, D, 512), BF), vm((3, D, H), F32),
            vm((6, CH, H), F32), vm((6, CH, H), BF), vm((6, CH, H), BF), vm((6, CH, H), BF), vm((3, CH, H), BF),
            vm((3, CH, 2 * BLK), BF), vm((3, CH, 2 * BLK), BF), vm((3, CH, BLK), BF), vm((6, CH, BLK), BF), vm((6, CH, 256), BF),
            dma((TA // 512,)), dma((6,)), dma((14,)), dma((14,)), dma((6,)), dma((6,)), dma((6,)), dma((3,)), dma((3,)),
            dma((3, 2)), dma((3, 2)), dma((3,)), dma((3,)), dma((3,)), dma((3,)), dma, dma, dma((2,)), dma((3,)), dma((3,)),
        ],
        compiler_params=pltpu.CompilerParams(collective_id=0, has_side_effects=True, vmem_limit_bytes=VMEM_LIMIT),
        name="gather_reduce_backward",
    )(x_t, dy_t, gate_shard.T, up_shard.T, down_shard, g_part.reshape(3 * D, H))
    dx_t, dw_local, dn_t = pl.pallas_call(
        kernel_b,
        out_shape=(shape((D, T), BF), shape((3, D, H), F32), shape((3, 192, D), F32)),
        in_specs=[ANY] * 6,
        out_specs=(ANY,) * 3,
        scratch_shapes=[
            vm((D, TB), BF), vm((D, TB), BF), vm((3, H, D), BF), vm((3, D, H), F32), vm((D, TA), BF), vm((3 * D, 256), BF),
            vm((256, D), F32), vm((3, 192, D), F32), vm((768, 512), BF), vm((768, 512), BF), vm((768, 512), BF),
            vm((D, TB), F32), vm((D, TB), BF),
            dma((TB // 256,)), dma((6,)), dma((2,)), dma((3,)), dma((12,)), dma((2,)),
        ],
        compiler_params=pltpu.CompilerParams(vmem_limit_bytes=VMEM_LIMIT),
        name="finish_backward",
    )(x_t, dy_t, w_all, dw_part, dx_part, sums.reshape(3 * D, 256))
    return dx_t.T, jnp.swapaxes(dn_t, 1, 2), dw_local[None]


def solution(mesh):
    return jax.shard_map(
        per_device,
        mesh=mesh,
        in_specs=(P(ALL_AXES, None), P(ALL_AXES, None), P(None, GROUP_AXES), P(None, GROUP_AXES), P(GROUP_AXES, None), P(ALL_AXES, None, None, None)),
        out_specs=(P(ALL_AXES, None), P(None, None, GROUP_AXES), P(ALL_AXES, None, None, None)),
        check_vma=False,
    )
```

```python
import jax
import jax.numpy as jnp
from jax import lax
from jax.experimental import pallas as pl
from jax.experimental.pallas import tpu as pltpu
from jax.sharding import PartitionSpec as P

ALL_AXES = ("dp", "row", "fsdp")
GROUP_AXES = ("row", "fsdp")
MESH = pl.DeviceIdType.MESH
NN = (((1,), (0,)), ((), ()))
NT = (((1,), (1,)), ((), ()))
TN = (((0,), (0,)), ((), ()))
F32 = jnp.float32
BF = jnp.bfloat16
ANY = pl.BlockSpec(memory_space=pl.ANY)
VM = pl.BlockSpec(memory_space=pltpu.VMEM)

D = 576
H = 1536
T = 4096
TA = 3072
TB = T - TA
CH = 144
BLK = 384
VMEM_LIMIT = 67043328
VMEM_A = 47 * 2**20
VMEM_B = 46 * 2**20
OWN_OUT, X_OUT, Y_OUT, OWN_MID, X_MID, Y_MID, DIAG = 0, 256, 512, 768, 896, 1024, 1152


def dot(lhs, rhs, dims):
    return lax.dot_general(lhs, rhs, dims, preferred_element_type=F32)


def forward_tile(x, dy, w, rows):
    a = dot(w[0, rows, :], x, NN)
    b = dot(w[1, rows, :], x, NN)
    dh = dot(w[2, rows, :], dy, NN)
    s = jax.nn.sigmoid(a)
    silu = a * s
    h = (silu * b).astype(BF)
    da = (dh * b * s * (1.0 + a * (1.0 - s))).astype(BF)
    db = (dh * silu).astype(BF)
    return h, da, db


def dx_tile(da, db, w, rows):
    return dot(w[0, rows, :], da, TN) + dot(w[1, rows, :], db, TN)


def kernel_a(
    x_hbm, dy_hbm, w1_hbm, w3_hbm, w2_hbm, g_hbm,
    w, dwa, dx_out, sum_out,
    xv, dv, da_s, db_s, h_s, dxa, dxo,
    stage, part, r0, acc, rz, r1, kept, r2, own, theirs,
    in_sem, wl_sem, ws, wr, st_sem, p_s, p_r, z_s, z_r, d1_s, d1_r, d2_s, d2_r, za_s, za_r, f_s, f_r, dxo_sem, dwo_sem, out_sem,
):
    dp = lax.axis_index("dp")
    row = lax.axis_index("row")
    f = lax.axis_index("fsdp")
    c = lax.rem(f, 2)
    x = f // 2
    fx = lax.rem(f + 2, 4)
    to_core = {"fsdp": f + 1 - 2 * c}
    to_x = {"fsdp": fx}
    to_y = {"row": 1 - row}
    to_z = {"dp": 1 - dp}
    to_xy = {"row": row + (1 - c) * (1 - 2 * row), "fsdp": f + c * (fx - f)}
    to_first = {"row": row + c * (1 - 2 * row), "fsdp": f + (1 - c) * (fx - f)}

    out_l, mid_l = 64 * c, 128 * (1 - c)

    def w_load(n):
        i, mid = n // 2, n % 2
        src = (w1_hbm, w3_hbm, w2_hbm)[i]
        if mid:
            return pltpu.make_async_copy(
                src.at[pl.ds(pl.multiple_of(mid_l, 64), 64), :], w.at[i, pl.ds(pl.multiple_of(OWN_MID + 64 * c, 64), 64), :], wl_sem.at[n]
            )
        return pltpu.make_async_copy(
            src.at[pl.ds(pl.multiple_of(out_l, 64), 128), :], w.at[i, pl.ds(pl.multiple_of(OWN_OUT + 128 * c, 128), 128), :], wl_sem.at[n]
        )

    def g_load(k, side):
        half = 1 - dp if k < 3 else dp
        core = c if side == 0 else 1 - c
        rows = pl.ds(pl.multiple_of(864 * core + 432 * half + CH * (k % 3), 16), CH)
        slot = 2 * (k % 3) + side
        return pltpu.make_async_copy(g_hbm.at[rows, :], stage.at[slot], st_sem.at[slot])

    def t_load(t, which):
        src, dst = ((x_hbm, xv), (dy_hbm, dv))[which]
        cols = pl.ds(t * 1024, 1024)
        return pltpu.make_async_copy(src.at[:, cols], dst.at[:, cols], in_sem.at[2 * t + which])

    for n in (0, 2, 4, 1, 3, 5):
        w_load(n).start()
    for k in range(3):
        g_load(k, 1).start()
        g_load(k, 0).start()
        if k == 0:
            t_load(0, 0).start()
            t_load(0, 1).start()
    for t in range(1, TA // 1024):
        t_load(t, 0).start()
        t_load(t, 1).start()

    barrier = pltpu.get_barrier_semaphore()
    for peer in (to_core, to_x, to_y, to_z):
        pl.semaphore_signal(barrier, inc=1, device_id=peer, device_id_type=MESH)
    for i in range(3):
        dwa[i] = jnp.zeros((D, H), F32)
    pl.semaphore_wait(barrier, 4)

    def w_rows(base, size):
        return w.at[:, pl.ds(pl.multiple_of(base, 64), size), :]

    def w_copy(n):
        o, m = 128 * c, 64 * c
        src, dst, size, peer = (
            (OWN_OUT + o, OWN_OUT + o, 128, to_core),
            (OWN_OUT + o, X_OUT + o, 128, to_x),
            (OWN_OUT + o, Y_OUT + o, 128, to_y),
            (OWN_MID + m, OWN_MID + m, 64, to_core),
            (OWN_MID + m, X_MID + m, 64, to_x),
            (OWN_MID + m, Y_MID + m, 64, to_y),
            (X_OUT + o, X_OUT + o, 128, to_core),
            (Y_OUT + o, Y_OUT + o, 128, to_core),
            (X_MID + m, X_MID + m, 64, to_core),
            (Y_MID + m, Y_MID + m, 64, to_core),
            (X_OUT + c * (Y_OUT + 128 - X_OUT), DIAG + 256 * c, 128, to_xy),
            (X_MID + c * (Y_MID + 64 - X_MID), DIAG + 128 + m, 64, to_xy),
            (DIAG + 256 * c, DIAG + 256 * c, 128, to_core),
            (DIAG + 128 + m, DIAG + 128 + m, 64, to_core),
        )[n]
        return pltpu.make_async_remote_copy(
            src_ref=w_rows(src, size), dst_ref=w_rows(dst, size), send_sem=ws.at[n], recv_sem=wr.at[n], device_id=peer, device_id_type=MESH
        )

    def w_send(*ns):
        for n in ns:
            w_copy(n).start()

    def w_arrived(*ns):
        for n in ns:
            w_copy(n).wait_recv()

    def remote(src, dst, s, r, peer):
        return pltpu.make_async_remote_copy(src_ref=src, dst_ref=dst, send_sem=s, recv_sem=r, device_id=peer, device_id_type=MESH)

    def p_copy(k):
        return remote(part.at[k], r0.at[k], p_s.at[k], p_r.at[k], to_core)

    def z_copy(k):
        return remote(acc.at[k], rz.at[k], z_s.at[k], z_r.at[k], to_z)

    def cols(q):
        return pl.ds(pl.multiple_of(q * BLK, BLK), BLK)

    def q_of(j, mine):
        on_x = 2 * j + (x if mine else 1 - x)
        on_y = 2 * (row if mine else 1 - row) + j
        return (1 - c) * on_x + c * on_y

    def d1_copy(k, j):
        return remote(acc.at[3 + k, :, cols(q_of(j, False))], r1.at[k, :, pl.ds(BLK * j, BLK)], d1_s.at[k, j], d1_r.at[k, j], to_first)

    m = (1 - c) * row + c * x

    def d2_copy(k):
        return remote(kept.at[k, :, cols(1 - m)], r2.at[k], d2_s.at[k], d2_r.at[k], to_xy)

    def za_copy(k):
        return remote(own.at[3 * dp + k], own.at[3 * dp + k], za_s.at[k], za_r.at[k], to_z)

    def za_arrival(k):
        return remote(own.at[3 * dp + k], own.at[3 * (1 - dp) + k], za_s.at[k], za_r.at[k], to_z)

    def lanes(core):
        return pl.ds(pl.multiple_of(128 * core, 128), 256)

    f_copy = remote(own.at[:, :, lanes(1 - c)], theirs, f_s, f_r, to_core)
    own_out = pltpu.make_async_copy(own.at[:, :, lanes(c)], sum_out.at[pl.ds(6 * c, 6)], out_sem.at[0])
    their_out = pltpu.make_async_copy(theirs, sum_out.at[pl.ds(6 * (1 - c), 6)], out_sem.at[1])

    def convert(base):
        for k in range(base, base + 3):
            g_load(k, 1).wait()
            part[k] = stage[2 * (k - base) + 1].astype(BF)
            g_load(k, 0).wait()
            acc[k] = stage[2 * (k - base)].astype(BF)
            if k > base:
                p_copy(k - 1).start()
        p_copy(base + 2).start()

    def add_partner(base):
        for k in range(base, base + 3):
            p_copy(k).wait_recv()
            acc[k] = acc[k] + r0[k]

    def z_step(k):
        z_copy(k).wait_recv()
        acc[3 + k] = acc[3 + k] + rz[k]
        d1_copy(k, 0).start()
        d1_copy(k, 1).start()

    def d1_step(k):
        for j in range(2):
            d1_copy(k, j).wait_recv()
        for j in range(2):
            at = pl.ds(BLK * j, BLK)
            kept[k, :, at] = acc[3 + k, :, cols(q_of(j, True))] + r1[k, :, at]
        d2_copy(k).start()

    def d2_step(k):
        d2_copy(k).wait_recv()
        own[3 * dp + k] = kept[k, :, cols(m)] + r2[k]
        za_copy(k).start()

    def dx_copy(t, size):
        at = pl.ds(pl.multiple_of(t * size, size), size)
        return pltpu.make_async_copy(dxo.at[lax.rem(t, 2)], dx_out.at[:, at], dxo_sem.at[lax.rem(t, 2)])

    def tile_step(base, size, t, tile, first, last):
        rows = pl.ds(base, size)
        at = pl.ds(pl.multiple_of(t * tile, tile), tile)
        xt, dyt = xv[:, at], dv[:, at]
        h_s[:size, :tile], da_s[:size, :tile], db_s[:size, :tile] = forward_tile(xt, dyt, w, rows)
        h, da, db = h_s[:size, :tile], da_s[:size, :tile], db_s[:size, :tile]
        dx = dx_tile(da, db, w, rows)
        if first:
            dxa[:, at] = dx
        elif last:
            dxo[lax.rem(t, 2)] = (dxa[:, at] + dx).astype(BF)
        else:
            dxa[:, at] += dx
        dwa[0, :, rows] += dot(xt, da, NT)
        dwa[1, :, rows] += dot(xt, db, NT)
        dwa[2, :, rows] += dot(dyt, h, NT)

    for n in (0, 2, 4):
        w_load(n).wait()
    w_send(0, 1, 2)
    for n in (1, 3, 5):
        w_load(n).wait()
    w_send(3, 4, 5)
    convert(0)
    for k in range(3, 6):
        g_load(k, 1).start()
        g_load(k, 0).start()
    w_arrived(0)

    @pl.loop(0, TA // 1024)
    def _(t):
        for i in range(TA // 1024):

            @pl.when(t == i)
            def _():
                t_load(i, 0).wait()
                t_load(i, 1).wait()

        @pl.when(t == 1)
        def _():
            convert(3)
            add_partner(0)
            for k in range(3):
                z_copy(k).start()

        tile_step(0, 256, t, 1024, True, False)

    w_arrived(1, 2)
    w_send(6, 7, 10)
    add_partner(3)
    w_arrived(6, 7)

    @pl.loop(0, TA // 1024)
    def _(t):
        @pl.when(t == 1)
        def _():
            w_arrived(3, 4, 5)
            w_send(8, 9, 11)
            z_step(0)

        @pl.when(t == 2)
        def _():
            w_arrived(10, 11)
            w_send(12, 13)
            d1_step(0)

        tile_step(256, 512, t, 1024, False, False)

    d2_step(0)
    w_arrived(8, 9, 12, 13)

    def g_output():
        for k in range(3):
            za_arrival(k).wait_recv()
        f_copy.start()
        own_out.start()

    def z2_d21():
        z_step(2)
        d2_step(1)

    @pl.loop(0, TA // 512)
    def _(t):
        steps = (lambda: z_step(1), lambda: d1_step(1), z2_d21, lambda: d1_step(2), lambda: d2_step(2), g_output)
        for i, step in enumerate(steps):
            pl.when(t == i)(step)

        @pl.when(t >= 2)
        def _():
            dx_copy(t - 2, 512).wait()

        tile_step(768, 768, t, 512, False, True)
        dx_copy(t, 512).start()

    f_copy.wait_recv()
    their_out.start()
    for t in (TA // 512 - 2, TA // 512 - 1):
        dx_copy(t, 512).wait()
    own_out.wait()
    their_out.wait()
    for n in range(14):
        w_copy(n).wait_send()
    for k in range(6):
        p_copy(k).wait_send()
    for k in range(3):
        z_copy(k).wait_send()
        d1_copy(k, 0).wait_send()
        d1_copy(k, 1).wait_send()
        d2_copy(k).wait_send()
        za_copy(k).wait_send()
    f_copy.wait_send()


def kernel_b(
    x_hbm, dy_hbm, w, dwp, dxp_hbm, sum_hbm,
    dx_out, dw_out, dn_out,
    xv, dv, dwa, dxp, sums, flip, dn, da_s, db_s, h_s, dxa, dxo,
    t_sem, misc_sem, dwo_sem, out_sem,
):
    row = lax.axis_index("row")
    f = lax.axis_index("fsdp")
    c = lax.rem(f, 2)
    x = f // 2
    q_own, q_x, q_y, q_d = 2 * row + x, 2 * row + 1 - x, 2 * (1 - row) + x, 2 * (1 - row) + 1 - x
    granule = [3 * q + j for q, j in (
        (q_own, 0), (q_own, 2), (q_x, 0), (q_x, 2), (q_y, 0), (q_y, 2), (q_own, 1), (q_x, 1), (q_y, 1), (q_d, 0), (q_d, 1), (q_d, 2)
    )]

    def t_load(t, which):
        src, dst = ((x_hbm, xv), (dy_hbm, dv))[which]
        return pltpu.make_async_copy(src.at[:, pl.ds(TA + 512 * t, 512)], dst.at[:, pl.ds(512 * t, 512)], t_sem.at[2 * t + which])

    sum_load = pltpu.make_async_copy(sum_hbm, sums, misc_sem.at[0])
    dxp_load = pltpu.make_async_copy(dxp_hbm, dxp, misc_sem.at[1])
    dxp_store = pltpu.make_async_copy(dxp, dx_out.at[:, pl.ds(0, TA)], misc_sem.at[2])
    dx_store = pltpu.make_async_copy(dxo, dx_out.at[:, pl.ds(TA, TB)], out_sem.at[0])
    dn_store = pltpu.make_async_copy(dn, dn_out, out_sem.at[1])

    t_load(0, 0).start()
    t_load(0, 1).start()
    t_load(1, 0).start()
    t_load(1, 1).start()
    sum_load.start()
    dxp_load.start()

    def dw_copy(k):
        at = pl.ds(pl.multiple_of(128 * granule[k], 128), 128)
        return pltpu.make_async_copy(dwa.at[:, :, pl.ds(128 * k, 128)], dw_out.at[:, :, at], dwo_sem.at[k])

    def tile_step(g, t, first):
        rows = pl.ds(768 * g, 768)
        at = pl.ds(pl.multiple_of(t * 512, 512), 512)
        xt, dyt = xv[:, at], dv[:, at]
        h_s[...], da_s[...], db_s[...] = forward_tile(xt, dyt, w, rows)
        h, da, db = h_s[...], da_s[...], db_s[...]
        dx = dx_tile(da, db, w, rows)
        if g == 0:
            dxa[:, at] = dx
        else:
            dxo[:, at] = (dxa[:, at] + dx).astype(BF)
        for i, (lhs, rhs) in enumerate(((xt, da), (xt, db), (dyt, h))):
            dwa[i, :, rows] = (dwp if first else dwa)[i, :, rows] + dot(lhs, rhs, NT)

    for t in range(2):
        for which in range(2):
            t_load(t, which).wait()
        tile_step(0, t, t == 0)
    for k in range(6):
        dw_copy(k).start()
    sum_load.wait()
    for i in range(3):
        flip[...] = jnp.transpose(sums[pl.ds(576 * i, 576), :].astype(F32))
        dn[i] = flip[pl.ds(pl.multiple_of(64 * c, 64), 192), :]
    dn_store.start()
    dxp_load.wait()
    dxp_store.start()

    for t in range(TB // 512):
        tile_step(1, t, t == 0)

    for k in range(6, 12):
        dw_copy(k).start()
    dx_store.start()
    for k in range(12):
        dw_copy(k).wait()
    dx_store.wait()
    dxp_store.wait()
    dn_store.wait()


def per_device(x_blk, dy_blk, gate_shard, up_shard, down_shard, g_part):
    x_t, dy_t = x_blk.T, dy_blk.T
    dma = pltpu.SemaphoreType.DMA
    vm = pltpu.VMEM
    shape = jax.ShapeDtypeStruct
    w_all, dw_part, dx_part, sums = pl.pallas_call(
        kernel_a,
        out_shape=(vm((3, H, D), BF), vm((3, D, H), F32), pltpu.HBM((D, TA), BF), pltpu.HBM((12, CH, 256), BF)),
        in_specs=[ANY] * 6,
        out_specs=(VM, VM, ANY, ANY),
        scratch_shapes=[
            vm((D, TA), BF), vm((D, TA), BF), vm((768, 1024), BF), vm((768, 1024), BF), vm((768, 1024), BF),
            vm((D, TA), F32), vm((2, D, 512), BF),
            vm((6, CH, H), F32), vm((6, CH, H), BF), vm((6, CH, H), BF), vm((6, CH, H), BF), vm((3, CH, H), BF),
            vm((3, CH, 2 * BLK), BF), vm((3, CH, 2 * BLK), BF), vm((3, CH, BLK), BF), vm((6, CH, BLK), BF), vm((6, CH, 256), BF),
            dma((TA // 512,)), dma((6,)), dma((14,)), dma((14,)), dma((6,)), dma((6,)), dma((6,)), dma((3,)), dma((3,)),
            dma((3, 2)), dma((3, 2)), dma((3,)), dma((3,)), dma((3,)), dma((3,)), dma, dma, dma((2,)), dma((3,)), dma((3,)),
        ],
        compiler_params=pltpu.CompilerParams(collective_id=0, has_side_effects=True, vmem_limit_bytes=VMEM_A),
        name="gather_reduce_backward",
    )(x_t, dy_t, gate_shard.T, up_shard.T, down_shard, g_part.reshape(3 * D, H))
    w_all = pltpu.with_memory_space_constraint(w_all, pltpu.VMEM)
    dw_part = pltpu.with_memory_space_constraint(dw_part, pltpu.VMEM)
    dx_t, dw_local, dn_t = pl.pallas_call(
        kernel_b,
        out_shape=(shape((D, T), BF), shape((3, D, H), F32), shape((3, 192, D), F32)),
        in_specs=[ANY, ANY, VM, VM, ANY, ANY],
        out_specs=(ANY,) * 3,
        scratch_shapes=[
            vm((D, TB), BF), vm((D, TB), BF), vm((3, D, H), F32), vm((D, TA), BF), vm((3 * D, 256), BF),
            vm((256, D), F32), vm((3, 192, D), F32), vm((768, 512), BF), vm((768, 512), BF), vm((768, 512), BF),
            vm((D, TB), F32), vm((D, TB), BF),
            dma((TB // 256,)), dma((3,)), dma((12,)), dma((2,)),
        ],
        compiler_params=pltpu.CompilerParams(vmem_limit_bytes=VMEM_B),
        name="finish_backward",
    )(x_t, dy_t, w_all, dw_part, dx_part, sums.reshape(3 * D, 256))
    return dx_t.T, jnp.swapaxes(dn_t, 1, 2), dw_local[None]


def solution(mesh):
    return jax.shard_map(
        per_device,
        mesh=mesh,
        in_specs=(P(ALL_AXES, None), P(ALL_AXES, None), P(None, GROUP_AXES), P(None, GROUP_AXES), P(GROUP_AXES, None), P(ALL_AXES, None, None, None)),
        out_specs=(P(ALL_AXES, None), P(None, None, GROUP_AXES), P(ALL_AXES, None, None, None)),
        check_vma=False,
    )
```

```python
import jax
import jax.numpy as jnp
from jax import lax
from jax.experimental import pallas as pl
from jax.experimental.pallas import tpu as pltpu
from jax.sharding import PartitionSpec as P

ALL_AXES = ("dp", "row", "fsdp")
GROUP_AXES = ("row", "fsdp")
MESH = pl.DeviceIdType.MESH
NN = (((1,), (0,)), ((), ()))
NT = (((1,), (1,)), ((), ()))
TN = (((0,), (0,)), ((), ()))
F32 = jnp.float32
BF = jnp.bfloat16
ANY = pl.BlockSpec(memory_space=pl.ANY)
VM = pl.BlockSpec(memory_space=pltpu.VMEM)

D = 576
H = 1536
T = 4096
TA = 3072
TB = T - TA
CH = 144
BLK = 384
VMEM_A = 37 * 2**20
VMEM_B = 37 * 2**20
OWN_OUT, X_OUT, Y_OUT, OWN_MID, X_MID, Y_MID, DIAG = 0, 256, 512, 768, 896, 1024, 1152


def dot(lhs, rhs, dims):
    return lax.dot_general(lhs, rhs, dims, preferred_element_type=F32)


def forward_tile(x, dy, w, rows):
    a = dot(w[0, rows, :], x, NN)
    b = dot(w[1, rows, :], x, NN)
    dh = dot(w[2, rows, :], dy, NN)
    s = jax.nn.sigmoid(a)
    silu = a * s
    h = (silu * b).astype(BF)
    da = (dh * b * s * (1.0 + a * (1.0 - s))).astype(BF)
    db = (dh * silu).astype(BF)
    return h, da, db


def dx_tile(da, db, w, rows):
    return dot(w[0, rows, :], da, TN) + dot(w[1, rows, :], db, TN)


def kernel_a(
    x_hbm, dy_hbm, w1_hbm, w3_hbm, w2_hbm, g_hbm,
    xv, dv, w, dwa, sums, dxo, dx_out, dx2_out,
    da_s, db_s, h_s, dxa,
    stage, part, r0, acc, rz, r1, kept, r2, own,
    in_sem, wl_sem, ws, wr, st_sem, p_s, p_r, z_s, z_r, d1_s, d1_r, d2_s, d2_r, za_s, za_r, f_s, f_r, dxo_sem, dx2_sem,
):
    dp = lax.axis_index("dp")
    row = lax.axis_index("row")
    f = lax.axis_index("fsdp")
    c = lax.rem(f, 2)
    x = f // 2
    fx = lax.rem(f + 2, 4)
    to_core = {"fsdp": f + 1 - 2 * c}
    to_x = {"fsdp": fx}
    to_y = {"row": 1 - row}
    to_z = {"dp": 1 - dp}
    to_xy = {"row": row + (1 - c) * (1 - 2 * row), "fsdp": f + c * (fx - f)}
    to_first = {"row": row + c * (1 - 2 * row), "fsdp": f + (1 - c) * (fx - f)}

    out_l, mid_l = 64 * c, 128 * (1 - c)

    def w_load(n):
        i, mid = n // 2, n % 2
        src = (w1_hbm, w3_hbm, w2_hbm)[i]
        if mid:
            return pltpu.make_async_copy(
                src.at[pl.ds(pl.multiple_of(mid_l, 64), 64), :], w.at[i, pl.ds(pl.multiple_of(OWN_MID + 64 * c, 64), 64), :], wl_sem.at[n]
            )
        return pltpu.make_async_copy(
            src.at[pl.ds(pl.multiple_of(out_l, 64), 128), :], w.at[i, pl.ds(pl.multiple_of(OWN_OUT + 128 * c, 128), 128), :], wl_sem.at[n]
        )

    def g_load(k, side):
        late = k // 3
        half = (1 - late) * (1 - dp) + late * dp
        core = c if side == 0 else 1 - c
        rows = pl.ds(pl.multiple_of(864 * core + 432 * half + CH * (k % 3), 16), CH)
        slot = 2 * (k % 2) + side
        return pltpu.make_async_copy(g_hbm.at[rows, :], stage.at[slot], st_sem.at[slot])

    def t_load(t, which):
        src, dst = ((x_hbm, xv), (dy_hbm, dv))[which]
        cols = pl.ds(pl.multiple_of(t * 1024, 1024), 1024)
        return pltpu.make_async_copy(src.at[:, cols], dst.at[:, cols], in_sem.at[2 * t + which])

    for n in (0, 2, 4, 1, 3, 5):
        w_load(n).start()
    t_load(3, 0).start()
    t_load(3, 1).start()
    for k in range(2):
        g_load(k, 1).start()
        g_load(k, 0).start()

    barrier = pltpu.get_barrier_semaphore()
    for peer in (to_core, to_x, to_y, to_z):
        pl.semaphore_signal(barrier, inc=1, device_id=peer, device_id_type=MESH)
    for i in range(3):
        dwa[i, :, :256] = jnp.zeros((D, 256), F32)
    pl.semaphore_wait(barrier, 4)

    def w_rows(base, size):
        return w.at[:, pl.ds(pl.multiple_of(base, 64), size), :]

    def w_copy(n):
        o, m = 128 * c, 64 * c
        src, dst, size, peer = (
            (OWN_OUT + o, OWN_OUT + o, 128, to_core),
            (OWN_OUT + o, X_OUT + o, 128, to_x),
            (OWN_OUT + o, Y_OUT + o, 128, to_y),
            (OWN_MID + m, OWN_MID + m, 64, to_core),
            (OWN_MID + m, X_MID + m, 64, to_x),
            (OWN_MID + m, Y_MID + m, 64, to_y),
            (X_OUT + o, X_OUT + o, 128, to_core),
            (Y_OUT + o, Y_OUT + o, 128, to_core),
            (X_MID + m, X_MID + m, 64, to_core),
            (Y_MID + m, Y_MID + m, 64, to_core),
            (X_OUT + c * (Y_OUT + 128 - X_OUT), DIAG + 256 * c, 128, to_xy),
            (X_MID + c * (Y_MID + 64 - X_MID), DIAG + 128 + m, 64, to_xy),
            (DIAG + 256 * c, DIAG + 256 * c, 128, to_core),
            (DIAG + 128 + m, DIAG + 128 + m, 64, to_core),
        )[n]
        return pltpu.make_async_remote_copy(
            src_ref=w_rows(src, size), dst_ref=w_rows(dst, size), send_sem=ws.at[n], recv_sem=wr.at[n], device_id=peer, device_id_type=MESH
        )

    def w_send(*ns):
        for n in ns:
            w_copy(n).start()

    def w_arrived(*ns):
        for n in ns:
            w_copy(n).wait_recv()

    def remote(src, dst, s, r, peer):
        return pltpu.make_async_remote_copy(src_ref=src, dst_ref=dst, send_sem=s, recv_sem=r, device_id=peer, device_id_type=MESH)

    def p_copy(k):
        return remote(part.at[k], r0.at[k], p_s.at[k], p_r.at[k], to_core)

    def z_copy(k):
        return remote(acc.at[k], rz.at[k], z_s.at[k], z_r.at[k], to_z)

    def cols(q):
        return pl.ds(pl.multiple_of(q * BLK, BLK), BLK)

    def q_of(j, mine):
        on_x = 2 * j + (x if mine else 1 - x)
        on_y = 2 * (row if mine else 1 - row) + j
        return (1 - c) * on_x + c * on_y

    def d1_copy(k, j):
        return remote(acc.at[3 + k, :, cols(q_of(j, False))], r1.at[k, :, pl.ds(BLK * j, BLK)], d1_s.at[k, j], d1_r.at[k, j], to_first)

    m = (1 - c) * row + c * x

    def d2_copy(k):
        return remote(kept.at[k, :, cols(1 - m)], r2.at[k], d2_s.at[k], d2_r.at[k], to_xy)

    def za_copy(k):
        return remote(own.at[3 * dp + k], own.at[3 * dp + k], za_s.at[k], za_r.at[k], to_z)

    def za_arrival(k):
        return remote(own.at[3 * dp + k], own.at[3 * (1 - dp) + k], za_s.at[k], za_r.at[k], to_z)

    def lanes(core):
        return pl.ds(pl.multiple_of(128 * core, 128), 256)

    f_copy = remote(own.at[:, :, lanes(1 - c)], sums.at[pl.ds(6 * c, 6)], f_s, f_r, to_core)
    f_arrival = remote(own.at[:, :, lanes(1 - c)], sums.at[pl.ds(6 * (1 - c), 6)], f_s, f_r, to_core)

    def convert(k):
        slot = 2 * (k % 2)
        part[k] = stage[slot + 1].astype(BF)
        acc[k] = stage[slot].astype(BF)

    def g_loaded(k):
        g_load(k, 1).wait()
        g_load(k, 0).wait()

    def z_step(k):
        p_copy(3 + k).wait_recv()
        z_copy(k).wait_recv()
        acc[3 + k] = acc[3 + k] + r0[3 + k] + rz[k]

    def d1_send(k):
        d1_copy(k, 0).start()
        d1_copy(k, 1).start()

    def d1_step(k):
        for j in range(2):
            d1_copy(k, j).wait_recv()
        for j in range(2):
            at = pl.ds(BLK * j, BLK)
            kept[k, :, at] = acc[3 + k, :, cols(q_of(j, True))] + r1[k, :, at]

    def d2_step(k):
        d2_copy(k).wait_recv()
        own[3 * dp + k] = kept[k, :, cols(m)] + r2[k]

    def dx_copy(t, size):
        at = pl.ds(pl.multiple_of(t * size, size), size)
        return pltpu.make_async_copy(dxo.at[lax.rem(t, 2)], dx_out.at[:, at], dxo_sem.at[lax.rem(t, 2)])

    dx2_copy = pltpu.make_async_copy(dxa.at[:, pl.ds(2048, TB)], dx2_out, dx2_sem)

    def tile_step(base, size, t, tile, put):
        rows = pl.ds(base, size)
        at = pl.ds(pl.multiple_of(t * tile, tile), tile)
        xt, dyt = xv[:, at], dv[:, at]
        h_s[:size, :tile], da_s[:size, :tile], db_s[:size, :tile] = forward_tile(xt, dyt, w, rows)
        h, da, db = h_s[:size, :tile], da_s[:size, :tile], db_s[:size, :tile]
        put(at, dx_tile(da, db, w, rows))
        dwa[0, :, rows] += dot(xt, da, NT)
        dwa[1, :, rows] += dot(xt, db, NT)
        dwa[2, :, rows] += dot(dyt, h, NT)

    for n in (0, 2, 4):
        w_load(n).wait()
    w_send(0, 1, 2)
    for n in (1, 3, 5):
        w_load(n).wait()
    w_send(3, 4, 5)
    w_arrived(0)

    def add_partner(k):
        p_copy(k).wait_recv()
        acc[k] = acc[k] + r0[k]

    @pl.loop(0, T // 1024)
    def _(t):
        @pl.when(t < 3)
        def _():
            t_load(t, 0).start()
            t_load(t, 1).start()

        @pl.when(t == 1)
        def _():
            dx2_copy.start()

        @pl.when(t > 1)
        def _():
            add_partner(t - 2)

        @pl.when(t > 0)
        def _():
            p_copy(t - 1).start()
            g_load(t + 1, 1).start()
            g_load(t + 1, 0).start()

        @pl.when(t > 1)
        def _():
            z_copy(t - 2).start()

        @pl.when(t == 3)
        def _():
            dx2_copy.wait()

        tt = lax.rem(t + 3, 4)
        t_load(tt, 0).wait()
        t_load(tt, 1).wait()
        g_loaded(t)
        convert(t)

        def put(at, dx):
            dxa[:, pl.ds(pl.multiple_of(1024 * lax.rem(t + 2, 3), 1024), 1024)] = dx

        tile_step(0, 256, tt, 1024, put)

    p_copy(3).start()
    w_arrived(1, 2)
    w_send(6, 7, 10)
    g_load(5, 1).start()
    g_load(5, 0).start()
    g_loaded(4)
    convert(4)
    add_partner(2)
    for i in range(3):
        dwa[i, :, 256:] = jnp.zeros((D, H - 256), F32)
    z_copy(2).start()
    p_copy(4).start()
    w_arrived(6, 7)

    def add_dx(at, dx):
        dxa[:, at] += dx

    @pl.loop(0, TA // 1024)
    def _(t):
        @pl.when(t == 1)
        def _():
            w_arrived(3, 4, 5)
            w_send(8, 9, 11)
            g_loaded(5)
            convert(5)
            z_step(0)
            p_copy(5).start()
            d1_send(0)

        @pl.when(t == 2)
        def _():
            w_arrived(10, 11)
            w_send(12, 13)
            d1_step(0)
            d2_copy(0).start()

        tile_step(256, 512, t, 1024, add_dx)

    d2_step(0)
    z_step(1)
    za_copy(0).start()
    d1_send(1)
    w_arrived(8, 9, 12, 13)

    def at_1():
        d1_step(1)
        d2_copy(1).start()

    def at_2():
        d2_step(1)
        z_step(2)
        za_copy(1).start()
        d1_send(2)

    def at_3():
        d1_step(2)
        d2_copy(2).start()

    def at_4():
        d2_step(2)
        za_copy(2).start()

    def at_5():
        for k in range(3):
            za_arrival(k).wait_recv()
        f_copy.start()
        sums[pl.ds(6 * c, 6)] = own[:, :, lanes(c)]

    @pl.loop(0, TA // 512)
    def _(t):
        for i, step in ((1, at_1), (2, at_2), (3, at_3), (4, at_4), (5, at_5)):
            pl.when(t == i)(step)

        @pl.when(t >= 2)
        def _():
            dx_copy(t - 2, 512).wait()

        def put(at, dx):
            dxo[lax.rem(t, 2)] = (dxa[:, at] + dx).astype(BF)

        tile_step(768, 768, t, 512, put)

        @pl.when(t < TA // 512 - 2)
        def _():
            dx_copy(t, 512).start()

    f_arrival.wait_recv()
    for n in range(14):
        w_copy(n).wait_send()
    for k in range(6):
        p_copy(k).wait_send()
    for k in range(3):
        z_copy(k).wait_send()
        d1_copy(k, 0).wait_send()
        d1_copy(k, 1).wait_send()
        d2_copy(k).wait_send()
        za_copy(k).wait_send()
    f_copy.wait_send()


def kernel_b(
    xv, dv, w, dwp, sums, dxo_a, dxp_hbm, dx2_hbm,
    dx_out, dw_out, dn_out,
    dwa, dxp, dx2, flip, dn, da_s, db_s, h_s, dxa, dxo,
    misc_sem, dw_sem, last_sem,
):
    row = lax.axis_index("row")
    f = lax.axis_index("fsdp")
    c = lax.rem(f, 2)
    x = f // 2
    q_own, q_x, q_y, q_d = 2 * row + x, 2 * row + 1 - x, 2 * (1 - row) + x, 2 * (1 - row) + 1 - x
    granule = [3 * q + j for q, j in (
        (q_own, 0), (q_own, 2), (q_x, 0), (q_x, 2), (q_y, 0), (q_y, 2), (q_own, 1), (q_x, 1), (q_y, 1), (q_d, 0), (q_d, 1), (q_d, 2)
    )]

    dxp_load = pltpu.make_async_copy(dxp_hbm, dxp, misc_sem.at[0])
    dxp_store = pltpu.make_async_copy(dxp, dx_out.at[:, pl.ds(0, TA - 1024)], misc_sem.at[1])
    dx2_load = pltpu.make_async_copy(dx2_hbm, dx2, misc_sem.at[2])
    dx_store = pltpu.make_async_copy(dxo, dx_out.at[:, pl.ds(TA, TB)], misc_sem.at[3])
    dn_store = pltpu.make_async_copy(dn, dn_out, misc_sem.at[4])

    def tail_store(i):
        return pltpu.make_async_copy(dxo_a.at[i], dx_out.at[:, pl.ds(TA - 1024 + 512 * i, 512)], misc_sem.at[5 + i])

    def place(k):
        return pl.ds(pl.multiple_of(128 * granule[k], 128), 128)

    def dw_copy(k):
        src = dwp if k < 2 else dwa
        return pltpu.make_async_copy(src.at[:, :, pl.ds(128 * k, 128)], dw_out.at[:, :, place(k)], dw_sem.at[k])

    def last_copy(i, k):
        return pltpu.make_async_copy(dwa.at[i, :, pl.ds(128 * k, 128)], dw_out.at[i, :, place(k)], last_sem.at[i, k - 2])

    for k in range(2):
        dw_copy(k).start()
    dxp_load.start()
    dx2_load.start()
    tail_store(0).start()
    tail_store(1).start()

    rows = pl.ds(768, 768)
    for t in range(2):
        mine, at = pl.ds(TA + 512 * t, 512), pl.ds(512 * t, 512)
        xt, dyt = xv[:, mine], dv[:, mine]
        h_s[:, :512], da_s[:, :512], db_s[:, :512] = forward_tile(xt, dyt, w, rows)
        h, da, db = h_s[:, :512], da_s[:, :512], db_s[:, :512]
        dxa[:, at] = dx_tile(da, db, w, rows)
        for i, (lhs, rhs) in enumerate(((xt, da), (xt, db), (dyt, h))):
            dwa[i, :, rows] = (dwp if t == 0 else dwa)[i, :, rows] + dot(lhs, rhs, NT)
    for k in range(6, 12):
        dw_copy(k).start()
    dxp_load.wait()
    dxp_store.start()
    dx2_load.wait()

    rows = pl.ds(256, 512)
    xt, dyt = xv[:, TA:], dv[:, TA:]
    for i in range(3):
        flip[i] = jnp.transpose(sums[4 * i : 4 * i + 4].reshape(D, 256).astype(F32))
        dn[i] = flip[i, pl.ds(pl.multiple_of(64 * c, 64), 192), :]
    h_s[:512], da_s[:512], db_s[:512] = forward_tile(xt, dyt, w, rows)
    h, da, db = h_s[:512], da_s[:512], db_s[:512]
    dxo[...] = (dxa[...] + dx2[...] + dx_tile(da, db, w, rows)).astype(BF)
    dx_store.start()
    dn_store.start()
    for i, (lhs, rhs) in enumerate(((xt, da), (xt, db), (dyt, h))):
        dwa[i, :, rows] = dwp[i, :, rows] + dot(lhs, rhs, NT)
        for k in range(2, 6):
            last_copy(i, k).start()

    for k in (0, 1, 6, 7, 8, 9, 10, 11):
        dw_copy(k).wait()
    dxp_store.wait()
    tail_store(0).wait()
    tail_store(1).wait()
    dx_store.wait()
    dn_store.wait()
    for i in range(3):
        for k in range(2, 6):
            last_copy(i, k).wait()


def per_device(x_blk, dy_blk, gate_shard, up_shard, down_shard, g_part):
    dma = pltpu.SemaphoreType.DMA
    vm, hbm = pltpu.VMEM, pltpu.HBM
    shape = jax.ShapeDtypeStruct
    *in_vmem, dx_part, dx2_part = pl.pallas_call(
        kernel_a,
        out_shape=(
            vm((D, T), BF), vm((D, T), BF), vm((3, H, D), BF), vm((3, D, H), F32), vm((12, CH, 256), BF), vm((2, D, 512), BF), hbm((D, TA - 1024), BF), hbm((D, TB), F32)
        ),
        in_specs=[ANY] * 6,
        out_specs=(VM,) * 6 + (ANY,) * 2,
        scratch_shapes=[
            vm((768, 1024), BF), vm((768, 1024), BF), vm((768, 1024), BF), vm((D, TA), F32),
            vm((4, CH, H), F32), vm((6, CH, H), BF), vm((6, CH, H), BF), vm((6, CH, H), BF), vm((3, CH, H), BF),
            vm((3, CH, 2 * BLK), BF), vm((3, CH, 2 * BLK), BF), vm((3, CH, BLK), BF), vm((6, CH, BLK), BF),
            dma((T // 512,)), dma((6,)), dma((14,)), dma((14,)), dma((4,)), dma((6,)), dma((6,)), dma((3,)), dma((3,)),
            dma((3, 2)), dma((3, 2)), dma((3,)), dma((3,)), dma((3,)), dma((3,)), dma, dma, dma((2,)), dma,
        ],
        compiler_params=pltpu.CompilerParams(collective_id=0, has_side_effects=True, vmem_limit_bytes=VMEM_A),
        name="gather_reduce_backward",
    )(x_blk.T, dy_blk.T, gate_shard.T, up_shard.T, down_shard, g_part.reshape(3 * D, H))
    in_vmem = [pltpu.with_memory_space_constraint(v, pltpu.VMEM) for v in in_vmem]
    dx_t, dw_local, dn_t = pl.pallas_call(
        kernel_b,
        out_shape=(shape((D, T), BF), shape((3, D, H), F32), shape((3, 192, D), F32)),
        in_specs=[VM] * 6 + [ANY] * 2,
        out_specs=(ANY,) * 3,
        scratch_shapes=[
            vm((3, D, H), F32), vm((D, TA - 1024), BF), vm((D, TB), F32), vm((3, 256, D), F32), vm((3, 192, D), F32),
            vm((768, TB), BF), vm((768, TB), BF), vm((768, TB), BF), vm((D, TB), F32), vm((D, TB), BF),
            dma((7,)), dma((12,)), dma((3, 4)),
        ],
        compiler_params=pltpu.CompilerParams(vmem_limit_bytes=VMEM_B),
        name="finish_backward",
    )(*in_vmem, dx_part, dx2_part)
    return dx_t.T, jnp.swapaxes(dn_t, 1, 2), dw_local[None]


def solution(mesh):
    return jax.shard_map(
        per_device,
        mesh=mesh,
        in_specs=(P(ALL_AXES, None), P(ALL_AXES, None), P(None, GROUP_AXES), P(None, GROUP_AXES), P(GROUP_AXES, None), P(ALL_AXES, None, None, None)),
        out_specs=(P(ALL_AXES, None), P(None, None, GROUP_AXES), P(ALL_AXES, None, None, None)),
        check_vma=False,
    )
```

```python
import jax
import jax.numpy as jnp
from jax import lax
from jax.experimental import pallas as pl
from jax.experimental.pallas import tpu as pltpu
from jax.sharding import PartitionSpec as P

ALL_AXES = ("dp", "row", "fsdp")
GROUP_AXES = ("row", "fsdp")
MESH = pl.DeviceIdType.MESH
NN = (((1,), (0,)), ((), ()))
NT = (((1,), (1,)), ((), ()))
TN = (((0,), (0,)), ((), ()))
F32 = jnp.float32
BF = jnp.bfloat16
ANY = pl.BlockSpec(memory_space=pl.ANY)
VM = pl.BlockSpec(memory_space=pltpu.VMEM)

D = 576
H = 1536
T = 4096
TA = 3072
TB = T - TA
CH = 144
BLK = 384
VMEM_A = 37 * 2**20
VMEM_B = 37 * 2**20
OWN_OUT, X_OUT, Y_OUT, OWN_MID, X_MID, Y_MID, DIAG = 0, 256, 512, 768, 896, 1024, 1152


def dot(lhs, rhs, dims):
    return lax.dot_general(lhs, rhs, dims, preferred_element_type=F32)


def forward_tile(x, dy, w, rows):
    a = dot(w[0, rows, :], x, NN)
    b = dot(w[1, rows, :], x, NN)
    dh = dot(w[2, rows, :], dy, NN)
    s = jax.nn.sigmoid(a)
    silu = a * s
    h = (silu * b).astype(BF)
    da = (dh * b * s * (1.0 + a * (1.0 - s))).astype(BF)
    db = (dh * silu).astype(BF)
    return h, da, db


def dx_tile(da, db, w, rows):
    return dot(w[0, rows, :], da, TN) + dot(w[1, rows, :], db, TN)


def kernel_a(
    x_hbm, dy_hbm, w1_hbm, w3_hbm, w2_hbm, g_hbm,
    xv, dv, w, dwa, sums, dxo, dx_out, dx2_out,
    da_s, db_s, h_s, dxa,
    stage, part, r0, acc, rz, r1, kept, r2, own,
    in_sem, wl_sem, ws, wr, st_sem, p_s, p_r, z_s, z_r, d1_s, d1_r, d2_s, d2_r, za_s, za_r, f_s, f_r, dxo_sem, dx2_sem,
):
    dp = lax.axis_index("dp")
    row = lax.axis_index("row")
    f = lax.axis_index("fsdp")
    c = lax.rem(f, 2)
    x = f // 2
    fx = lax.rem(f + 2, 4)
    to_core = {"fsdp": f + 1 - 2 * c}
    to_x = {"fsdp": fx}
    to_y = {"row": 1 - row}
    to_z = {"dp": 1 - dp}
    to_xy = {"row": row + (1 - c) * (1 - 2 * row), "fsdp": f + c * (fx - f)}
    to_first = {"row": row + c * (1 - 2 * row), "fsdp": f + (1 - c) * (fx - f)}

    out_l, mid_l = 64 * c, 128 * (1 - c)

    def w_load(n):
        i, mid = n // 2, n % 2
        src = (w1_hbm, w3_hbm, w2_hbm)[i]
        if mid:
            return pltpu.make_async_copy(
                src.at[pl.ds(pl.multiple_of(mid_l, 64), 64), :], w.at[i, pl.ds(pl.multiple_of(OWN_MID + 64 * c, 64), 64), :], wl_sem.at[n]
            )
        return pltpu.make_async_copy(
            src.at[pl.ds(pl.multiple_of(out_l, 64), 128), :], w.at[i, pl.ds(pl.multiple_of(OWN_OUT + 128 * c, 128), 128), :], wl_sem.at[n]
        )

    def g_load(k, side):
        late = k // 3
        half = (1 - late) * (1 - dp) + late * dp
        core = c if side == 0 else 1 - c
        rows = pl.ds(pl.multiple_of(864 * core + 432 * half + CH * (k % 3), 16), CH)
        slot = 2 * (k % 2) + side
        return pltpu.make_async_copy(g_hbm.at[rows, :], stage.at[slot], st_sem.at[slot])

    def t_load(t, which):
        src, dst = ((x_hbm, xv), (dy_hbm, dv))[which]
        cols = pl.ds(pl.multiple_of(t * 1024, 1024), 1024)
        return pltpu.make_async_copy(src.at[:, cols], dst.at[:, cols], in_sem.at[2 * t + which])

    for n in (0, 2, 4, 1, 3, 5):
        w_load(n).start()
    t_load(3, 0).start()
    t_load(3, 1).start()
    for k in range(2):
        g_load(k, 1).start()
        g_load(k, 0).start()

    barrier = pltpu.get_barrier_semaphore()
    for peer in (to_core, to_x, to_y, to_z):
        pl.semaphore_signal(barrier, inc=1, device_id=peer, device_id_type=MESH)
    for i in range(3):
        dwa[i] = jnp.zeros((D, H), F32)
    pl.semaphore_wait(barrier, 4)

    def w_rows(base, size):
        return w.at[:, pl.ds(pl.multiple_of(base, 64), size), :]

    def w_copy(n):
        o, m = 128 * c, 64 * c
        src, dst, size, peer = (
            (OWN_OUT + o, OWN_OUT + o, 128, to_core),
            (OWN_OUT + o, X_OUT + o, 128, to_x),
            (OWN_OUT + o, Y_OUT + o, 128, to_y),
            (OWN_MID + m, OWN_MID + m, 64, to_core),
            (OWN_MID + m, X_MID + m, 64, to_x),
            (OWN_MID + m, Y_MID + m, 64, to_y),
            (X_OUT + o, X_OUT + o, 128, to_core),
            (Y_OUT + o, Y_OUT + o, 128, to_core),
            (X_MID + m, X_MID + m, 64, to_core),
            (Y_MID + m, Y_MID + m, 64, to_core),
            (X_OUT + c * (Y_OUT + 128 - X_OUT), DIAG + 256 * c, 128, to_xy),
            (X_MID + c * (Y_MID + 64 - X_MID), DIAG + 128 + m, 64, to_xy),
            (DIAG + 256 * c, DIAG + 256 * c, 128, to_core),
            (DIAG + 128 + m, DIAG + 128 + m, 64, to_core),
        )[n]
        return pltpu.make_async_remote_copy(
            src_ref=w_rows(src, size), dst_ref=w_rows(dst, size), send_sem=ws.at[n], recv_sem=wr.at[n], device_id=peer, device_id_type=MESH
        )

    def w_send(*ns):
        for n in ns:
            w_copy(n).start()

    def w_arrived(*ns):
        for n in ns:
            w_copy(n).wait_recv()

    def remote(src, dst, s, r, peer):
        return pltpu.make_async_remote_copy(src_ref=src, dst_ref=dst, send_sem=s, recv_sem=r, device_id=peer, device_id_type=MESH)

    def p_copy(k):
        return remote(part.at[k], r0.at[k], p_s.at[k], p_r.at[k], to_core)

    def z_copy(k):
        return remote(acc.at[k], rz.at[k], z_s.at[k], z_r.at[k], to_z)

    def cols(q):
        return pl.ds(pl.multiple_of(q * BLK, BLK), BLK)

    def q_of(j, mine):
        on_x = 2 * j + (x if mine else 1 - x)
        on_y = 2 * (row if mine else 1 - row) + j
        return (1 - c) * on_x + c * on_y

    def d1_copy(k, j):
        return remote(acc.at[3 + k, :, cols(q_of(j, False))], r1.at[k, :, pl.ds(BLK * j, BLK)], d1_s.at[k, j], d1_r.at[k, j], to_first)

    m = (1 - c) * row + c * x

    def d2_copy(k):
        return remote(kept.at[k, :, cols(1 - m)], r2.at[k], d2_s.at[k], d2_r.at[k], to_xy)

    def za_copy(k):
        return remote(own.at[3 * dp + k], own.at[3 * dp + k], za_s.at[k], za_r.at[k], to_z)

    def za_arrival(k):
        return remote(own.at[3 * dp + k], own.at[3 * (1 - dp) + k], za_s.at[k], za_r.at[k], to_z)

    def lanes(core):
        return pl.ds(pl.multiple_of(128 * core, 128), 256)

    f_copy = remote(own.at[:, :, lanes(1 - c)], sums.at[pl.ds(6 * c, 6)], f_s, f_r, to_core)
    f_arrival = remote(own.at[:, :, lanes(1 - c)], sums.at[pl.ds(6 * (1 - c), 6)], f_s, f_r, to_core)

    def convert(k):
        slot = 2 * (k % 2)
        part[k] = stage[slot + 1].astype(BF)
        acc[k] = stage[slot].astype(BF)

    def g_loaded(k):
        g_load(k, 1).wait()
        g_load(k, 0).wait()

    def z_step(k):
        p_copy(3 + k).wait_recv()
        z_copy(k).wait_recv()
        acc[3 + k] = acc[3 + k] + r0[3 + k] + rz[k]

    def d1_send(k):
        d1_copy(k, 0).start()
        d1_copy(k, 1).start()

    def d1_step(k):
        for j in range(2):
            d1_copy(k, j).wait_recv()
        for j in range(2):
            at = pl.ds(BLK * j, BLK)
            kept[k, :, at] = acc[3 + k, :, cols(q_of(j, True))] + r1[k, :, at]

    def d2_step(k):
        d2_copy(k).wait_recv()
        own[3 * dp + k] = kept[k, :, cols(m)] + r2[k]

    def dx_copy(t, size):
        at = pl.ds(pl.multiple_of(t * size, size), size)
        return pltpu.make_async_copy(dxo.at[lax.rem(t, 2)], dx_out.at[:, at], dxo_sem.at[lax.rem(t, 2)])

    dx2_copy = pltpu.make_async_copy(dxa.at[:, pl.ds(2048, TB)], dx2_out, dx2_sem)

    def tile_step(base, size, t, tile, put, parts=1):
        rows = pl.ds(base, size)
        at = pl.ds(pl.multiple_of(t * tile, tile), tile)
        sub = tile // parts
        for j in range(parts):
            ats = pl.ds(pl.multiple_of(t * tile + j * sub, sub), sub)
            cut = slice(j * sub, (j + 1) * sub)
            h_s[:size, cut], da_s[:size, cut], db_s[:size, cut] = forward_tile(xv[:, ats], dv[:, ats], w, rows)
        for j in range(parts):
            cut = slice(j * sub, (j + 1) * sub)
            put(j * sub, sub, dx_tile(da_s[:size, cut], db_s[:size, cut], w, rows))
        xt, dyt = xv[:, at], dv[:, at]
        h, da, db = h_s[:size, :tile], da_s[:size, :tile], db_s[:size, :tile]
        dwa[0, :, rows] += dot(xt, da, NT)
        dwa[1, :, rows] += dot(xt, db, NT)
        dwa[2, :, rows] += dot(dyt, h, NT)

    for n in (0, 2, 4):
        w_load(n).wait()
    w_send(0, 1, 2)
    for n in (1, 3, 5):
        w_load(n).wait()
    w_send(3, 4, 5)
    g_loaded(0)
    convert(0)
    g_load(2, 1).start()
    g_load(2, 0).start()
    p_copy(0).start()
    w_arrived(0)

    def add_partner(k):
        p_copy(k).wait_recv()
        acc[k] = acc[k] + r0[k]

    @pl.loop(0, T // 1024)
    def _(t):
        @pl.when(t < 3)
        def _():
            t_load(t, 0).start()
            t_load(t, 1).start()

        @pl.when(t == 1)
        def _():
            dx2_copy.start()

        @pl.when(t > 0)
        def _():
            add_partner(t - 1)
            p_copy(t).start()
            g_load(t + 2, 1).start()
            g_load(t + 2, 0).start()
            z_copy(t - 1).start()

        @pl.when(t == 3)
        def _():
            dx2_copy.wait()
            w_arrived(1, 2)
            w_send(6, 7, 10)

        tt = lax.rem(t + 3, 4)
        t_load(tt, 0).wait()
        t_load(tt, 1).wait()
        g_loaded(t + 1)
        convert(t + 1)

        def put(off, sub, dx):
            dxa[:, pl.ds(pl.multiple_of(1024 * lax.rem(t + 2, 3) + off, 256), sub)] = dx

        tile_step(0, 256, tt, 1024, put, 4)

    p_copy(4).start()
    g_loaded(5)
    convert(5)
    w_arrived(6, 7)

    @pl.loop(0, TA // 1024)
    def _(t):
        @pl.when(t == 1)
        def _():
            w_arrived(3, 4, 5)
            w_send(8, 9, 11)
            p_copy(5).start()

        @pl.when(t == 2)
        def _():
            w_arrived(10, 11)
            w_send(12, 13)
            z_step(0)
            d1_send(0)

        def put(off, sub, dx):
            dxa[:, pl.ds(pl.multiple_of(1024 * t + off, 256), sub)] += dx

        tile_step(256, 512, t, 1024, put, 4)

    d1_step(0)
    z_step(1)
    d2_copy(0).start()
    d1_send(1)
    w_arrived(8, 9, 12, 13)

    def at_1():
        d2_step(0)
        d1_step(1)
        za_copy(0).start()
        d2_copy(1).start()

    def at_2():
        d2_step(1)
        z_step(2)
        za_copy(1).start()
        d1_send(2)

    def at_3():
        d1_step(2)
        d2_copy(2).start()

    def at_4():
        d2_step(2)
        za_copy(2).start()

    def at_5():
        for k in range(3):
            za_arrival(k).wait_recv()
        f_copy.start()
        sums[pl.ds(6 * c, 6)] = own[:, :, lanes(c)]

    @pl.loop(0, TA // 512)
    def _(t):
        for i, step in ((1, at_1), (2, at_2), (3, at_3), (4, at_4), (5, at_5)):
            pl.when(t == i)(step)

        @pl.when(t >= 2)
        def _():
            dx_copy(t - 2, 512).wait()

        def put(off, sub, dx):
            dxo[lax.rem(t, 2)] = (dxa[:, pl.ds(pl.multiple_of(512 * t, 512), 512)] + dx).astype(BF)

        tile_step(768, 768, t, 512, put)

        @pl.when(t < TA // 512 - 2)
        def _():
            dx_copy(t, 512).start()

    f_arrival.wait_recv()
    for n in range(14):
        w_copy(n).wait_send()
    for k in range(6):
        p_copy(k).wait_send()
    for k in range(3):
        z_copy(k).wait_send()
        d1_copy(k, 0).wait_send()
        d1_copy(k, 1).wait_send()
        d2_copy(k).wait_send()
        za_copy(k).wait_send()
    f_copy.wait_send()


def kernel_b(
    xv, dv, w, dwp, sums, dxo_a, dxp_hbm, dx2_hbm,
    dx_out, dw_out, dn_out,
    dwa, dxp, dx2, flip, dn, da_s, db_s, h_s, dxa, dxo,
    misc_sem, dw_sem, last_sem,
):
    row = lax.axis_index("row")
    f = lax.axis_index("fsdp")
    c = lax.rem(f, 2)
    x = f // 2
    q_own, q_x, q_y, q_d = 2 * row + x, 2 * row + 1 - x, 2 * (1 - row) + x, 2 * (1 - row) + 1 - x
    granule = [3 * q + j for q, j in (
        (q_own, 0), (q_own, 2), (q_x, 0), (q_x, 2), (q_y, 0), (q_y, 2), (q_own, 1), (q_x, 1), (q_y, 1), (q_d, 0), (q_d, 1), (q_d, 2)
    )]

    dxp_load = pltpu.make_async_copy(dxp_hbm, dxp, misc_sem.at[0])
    dxp_store = pltpu.make_async_copy(dxp, dx_out.at[:, pl.ds(0, TA - 1024)], misc_sem.at[1])
    dx2_load = pltpu.make_async_copy(dx2_hbm, dx2, misc_sem.at[2])
    dx_store = pltpu.make_async_copy(dxo, dx_out.at[:, pl.ds(TA, TB)], misc_sem.at[3])
    dn_store = pltpu.make_async_copy(dn, dn_out, misc_sem.at[4])

    def tail_store(i):
        return pltpu.make_async_copy(dxo_a.at[i], dx_out.at[:, pl.ds(TA - 1024 + 512 * i, 512)], misc_sem.at[5 + i])

    def place(k):
        return pl.ds(pl.multiple_of(128 * granule[k], 128), 128)

    def dw_copy(k):
        src = dwp if k < 2 else dwa
        return pltpu.make_async_copy(src.at[:, :, pl.ds(128 * k, 128)], dw_out.at[:, :, place(k)], dw_sem.at[k])

    def last_copy(i, k):
        return pltpu.make_async_copy(dwa.at[i, :, pl.ds(128 * k, 128)], dw_out.at[i, :, place(k)], last_sem.at[i, k - 2])

    for k in range(2):
        dw_copy(k).start()
    dxp_load.start()
    dx2_load.start()
    tail_store(0).start()
    tail_store(1).start()

    rows = pl.ds(768, 768)
    for t in range(2):
        mine, at = pl.ds(TA + 512 * t, 512), pl.ds(512 * t, 512)
        xt, dyt = xv[:, mine], dv[:, mine]
        h_s[:, :512], da_s[:, :512], db_s[:, :512] = forward_tile(xt, dyt, w, rows)
        h, da, db = h_s[:, :512], da_s[:, :512], db_s[:, :512]
        dxa[:, at] = dx_tile(da, db, w, rows)
        for i, (lhs, rhs) in enumerate(((xt, da), (xt, db), (dyt, h))):
            dwa[i, :, rows] = (dwp if t == 0 else dwa)[i, :, rows] + dot(lhs, rhs, NT)
    for k in range(6, 12):
        dw_copy(k).start()
    dxp_load.wait()
    dxp_store.start()
    dx2_load.wait()

    rows = pl.ds(256, 512)
    xt, dyt = xv[:, TA:], dv[:, TA:]
    for i in range(3):
        flip[i] = jnp.transpose(sums[4 * i : 4 * i + 4].reshape(D, 256).astype(F32))
        dn[i] = flip[i, pl.ds(pl.multiple_of(64 * c, 64), 192), :]
    cuts = [slice(j, j + 256) for j in range(0, TB, 256)]
    for cut in cuts:
        h_s[:512, cut], da_s[:512, cut], db_s[:512, cut] = forward_tile(xt[:, cut], dyt[:, cut], w, rows)
    for cut in cuts:
        dxo[:, cut] = (dxa[:, cut] + dx2[:, cut] + dx_tile(da_s[:512, cut], db_s[:512, cut], w, rows)).astype(BF)
    h, da, db = h_s[:512], da_s[:512], db_s[:512]
    dx_store.start()
    dn_store.start()
    for i, (lhs, rhs) in enumerate(((xt, da), (xt, db), (dyt, h))):
        dwa[i, :, rows] = dwp[i, :, rows] + dot(lhs, rhs, NT)
        for k in range(2, 6):
            last_copy(i, k).start()

    for k in (0, 1, 6, 7, 8, 9, 10, 11):
        dw_copy(k).wait()
    dxp_store.wait()
    tail_store(0).wait()
    tail_store(1).wait()
    dx_store.wait()
    dn_store.wait()
    for i in range(3):
        for k in range(2, 6):
            last_copy(i, k).wait()


def per_device(x_blk, dy_blk, gate_shard, up_shard, down_shard, g_part):
    dma = pltpu.SemaphoreType.DMA
    vm, hbm = pltpu.VMEM, pltpu.HBM
    shape = jax.ShapeDtypeStruct
    *in_vmem, dx_part, dx2_part = pl.pallas_call(
        kernel_a,
        out_shape=(
            vm((D, T), BF), vm((D, T), BF), vm((3, H, D), BF), vm((3, D, H), F32), vm((12, CH, 256), BF), vm((2, D, 512), BF), hbm((D, TA - 1024), BF), hbm((D, TB), F32)
        ),
        in_specs=[ANY] * 6,
        out_specs=(VM,) * 6 + (ANY,) * 2,
        scratch_shapes=[
            vm((768, 1024), BF), vm((768, 1024), BF), vm((768, 1024), BF), vm((D, TA), F32),
            vm((4, CH, H), F32), vm((6, CH, H), BF), vm((6, CH, H), BF), vm((6, CH, H), BF), vm((3, CH, H), BF),
            vm((3, CH, 2 * BLK), BF), vm((3, CH, 2 * BLK), BF), vm((3, CH, BLK), BF), vm((6, CH, BLK), BF),
            dma((T // 512,)), dma((6,)), dma((14,)), dma((14,)), dma((4,)), dma((6,)), dma((6,)), dma((3,)), dma((3,)),
            dma((3, 2)), dma((3, 2)), dma((3,)), dma((3,)), dma((3,)), dma((3,)), dma, dma, dma((2,)), dma,
        ],
        compiler_params=pltpu.CompilerParams(collective_id=0, has_side_effects=True, vmem_limit_bytes=VMEM_A),
        name="gather_reduce_backward",
    )(x_blk.T, dy_blk.T, gate_shard.T, up_shard.T, down_shard, g_part.reshape(3 * D, H))
    in_vmem = [pltpu.with_memory_space_constraint(v, pltpu.VMEM) for v in in_vmem]
    dx_t, dw_local, dn_t = pl.pallas_call(
        kernel_b,
        out_shape=(shape((D, T), BF), shape((3, D, H), F32), shape((3, 192, D), F32)),
        in_specs=[VM] * 6 + [ANY] * 2,
        out_specs=(ANY,) * 3,
        scratch_shapes=[
            vm((3, D, H), F32), vm((D, TA - 1024), BF), vm((D, TB), F32), vm((3, 256, D), F32), vm((3, 192, D), F32),
            vm((768, TB), BF), vm((768, TB), BF), vm((768, TB), BF), vm((D, TB), F32), vm((D, TB), BF),
            dma((7,)), dma((12,)), dma((3, 4)),
        ],
        compiler_params=pltpu.CompilerParams(vmem_limit_bytes=VMEM_B),
        name="finish_backward",
    )(*in_vmem, dx_part, dx2_part)
    return dx_t.T, jnp.swapaxes(dn_t, 1, 2), dw_local[None]


def solution(mesh):
    return jax.shard_map(
        per_device,
        mesh=mesh,
        in_specs=(P(ALL_AXES, None), P(ALL_AXES, None), P(None, GROUP_AXES), P(None, GROUP_AXES), P(GROUP_AXES, None), P(ALL_AXES, None, None, None)),
        out_specs=(P(ALL_AXES, None), P(None, None, GROUP_AXES), P(ALL_AXES, None, None, None)),
        check_vma=False,
    )
```

```python
import jax
import jax.numpy as jnp
from jax import lax
from jax.experimental import pallas as pl
from jax.experimental.pallas import tpu as pltpu
from jax.sharding import PartitionSpec as P

ALL_AXES = ("dp", "row", "fsdp")
GROUP_AXES = ("row", "fsdp")
MESH = pl.DeviceIdType.MESH
NN = (((1,), (0,)), ((), ()))
NT = (((1,), (1,)), ((), ()))
TN = (((0,), (0,)), ((), ()))
F32 = jnp.float32
BF = jnp.bfloat16
ANY = pl.BlockSpec(memory_space=pl.ANY)
VM = pl.BlockSpec(memory_space=pltpu.VMEM)

D = 576
H = 1536
T = 4096
TA = 3072
TB = T - TA
CH = 144
BLK = 384
VMEM_A = 37 * 2**20
VMEM_B = 37 * 2**20
OWN_OUT, X_OUT, Y_OUT, OWN_MID, X_MID, Y_MID, DIAG = 0, 256, 512, 768, 896, 1024, 1152


def dot(lhs, rhs, dims):
    return lax.dot_general(lhs, rhs, dims, preferred_element_type=F32)


def forward_tile(x, dy, w, rows):
    a = dot(w[0, rows, :], x, NN)
    b = dot(w[1, rows, :], x, NN)
    dh = dot(w[2, rows, :], dy, NN)
    s = jax.nn.sigmoid(a)
    silu = a * s
    h = (silu * b).astype(BF)
    da = (dh * b * s * (1.0 + a * (1.0 - s))).astype(BF)
    db = (dh * silu).astype(BF)
    return h, da, db


def dx_tile(da, db, w, rows):
    return dot(w[0, rows, :], da, TN) + dot(w[1, rows, :], db, TN)


def kernel_a(
    x_hbm, dy_hbm, w1_hbm, w3_hbm, w2_hbm, g_hbm,
    xv, dv, w, dwa, sums, dxo, dx_out, dx2_out,
    da_s, db_s, h_s, dxa,
    stage, part, r0, acc, rz, r1, kept, r2, own,
    in_sem, wl_sem, ws, wr, st_sem, p_s, p_r, z_s, z_r, d1_s, d1_r, d2_s, d2_r, za_s, za_r, f_s, f_r, dxo_sem, dx2_sem,
):
    dp = lax.axis_index("dp")
    row = lax.axis_index("row")
    f = lax.axis_index("fsdp")
    c = lax.rem(f, 2)
    x = f // 2
    fx = lax.rem(f + 2, 4)
    to_core = {"fsdp": f + 1 - 2 * c}
    to_x = {"fsdp": fx}
    to_y = {"row": 1 - row}
    to_z = {"dp": 1 - dp}
    to_xy = {"row": row + (1 - c) * (1 - 2 * row), "fsdp": f + c * (fx - f)}
    to_first = {"row": row + c * (1 - 2 * row), "fsdp": f + (1 - c) * (fx - f)}

    out_l, mid_l = 64 * c, 128 * (1 - c)

    def w_load(n):
        i, mid = n // 2, n % 2
        src = (w1_hbm, w3_hbm, w2_hbm)[i]
        if mid:
            return pltpu.make_async_copy(
                src.at[pl.ds(pl.multiple_of(mid_l, 64), 64), :], w.at[i, pl.ds(pl.multiple_of(OWN_MID + 64 * c, 64), 64), :], wl_sem.at[n]
            )
        return pltpu.make_async_copy(
            src.at[pl.ds(pl.multiple_of(out_l, 64), 128), :], w.at[i, pl.ds(pl.multiple_of(OWN_OUT + 128 * c, 128), 128), :], wl_sem.at[n]
        )

    def g_load(k, side):
        late = k // 3
        half = (1 - late) * (1 - dp) + late * dp
        core = c if side == 0 else 1 - c
        rows = pl.ds(pl.multiple_of(864 * core + 432 * half + CH * (k % 3), 16), CH)
        slot = 2 * (k % 2) + side
        return pltpu.make_async_copy(g_hbm.at[rows, :], stage.at[slot], st_sem.at[slot])

    def t_load(t, which):
        src, dst = ((x_hbm, xv), (dy_hbm, dv))[which]
        cols = pl.ds(pl.multiple_of(t * 1024, 1024), 1024)
        return pltpu.make_async_copy(src.at[:, cols], dst.at[:, cols], in_sem.at[2 * t + which])

    for n in (0, 2, 4, 1, 3, 5):
        w_load(n).start()
    t_load(3, 0).start()
    t_load(3, 1).start()
    for k in range(2):
        g_load(k, 1).start()
        g_load(k, 0).start()

    barrier = pltpu.get_barrier_semaphore()
    for peer in (to_core, to_x, to_y, to_z):
        pl.semaphore_signal(barrier, inc=1, device_id=peer, device_id_type=MESH)
    for i in range(3):
        dwa[i] = jnp.zeros((D, H), F32)
    pl.semaphore_wait(barrier, 4)

    def w_rows(base, size):
        return w.at[:, pl.ds(pl.multiple_of(base, 64), size), :]

    def w_copy(n):
        o, m = 128 * c, 64 * c
        src, dst, size, peer = (
            (OWN_OUT + o, OWN_OUT + o, 128, to_core),
            (OWN_OUT + o, X_OUT + o, 128, to_x),
            (OWN_OUT + o, Y_OUT + o, 128, to_y),
            (OWN_MID + m, OWN_MID + m, 64, to_core),
            (OWN_MID + m, X_MID + m, 64, to_x),
            (OWN_MID + m, Y_MID + m, 64, to_y),
            (X_OUT + o, X_OUT + o, 128, to_core),
            (Y_OUT + o, Y_OUT + o, 128, to_core),
            (X_MID + m, X_MID + m, 64, to_core),
            (Y_MID + m, Y_MID + m, 64, to_core),
            (X_OUT + c * (Y_OUT + 128 - X_OUT), DIAG + 256 * c, 128, to_xy),
            (X_MID + c * (Y_MID + 64 - X_MID), DIAG + 128 + m, 64, to_xy),
            (DIAG + 256 * c, DIAG + 256 * c, 128, to_core),
            (DIAG + 128 + m, DIAG + 128 + m, 64, to_core),
        )[n]
        return pltpu.make_async_remote_copy(
            src_ref=w_rows(src, size), dst_ref=w_rows(dst, size), send_sem=ws.at[n], recv_sem=wr.at[n], device_id=peer, device_id_type=MESH
        )

    def w_send(*ns):
        for n in ns:
            w_copy(n).start()

    def w_arrived(*ns):
        for n in ns:
            w_copy(n).wait_recv()

    def remote(src, dst, s, r, peer):
        return pltpu.make_async_remote_copy(src_ref=src, dst_ref=dst, send_sem=s, recv_sem=r, device_id=peer, device_id_type=MESH)

    def p_copy(k):
        return remote(part.at[k], r0.at[k], p_s.at[k], p_r.at[k], to_core)

    def z_copy(k):
        return remote(acc.at[k], rz.at[k], z_s.at[k], z_r.at[k], to_z)

    def cols(q):
        return pl.ds(pl.multiple_of(q * BLK, BLK), BLK)

    def q_of(j, mine):
        on_x = 2 * j + (x if mine else 1 - x)
        on_y = 2 * (row if mine else 1 - row) + j
        return (1 - c) * on_x + c * on_y

    def d1_copy(k, j):
        return remote(acc.at[3 + k, :, cols(q_of(j, False))], r1.at[k, :, pl.ds(BLK * j, BLK)], d1_s.at[k, j], d1_r.at[k, j], to_first)

    m = (1 - c) * row + c * x

    def d2_copy(k):
        return remote(kept.at[k, :, cols(1 - m)], r2.at[k], d2_s.at[k], d2_r.at[k], to_xy)

    def za_copy(k):
        return remote(own.at[3 * dp + k], own.at[3 * dp + k], za_s.at[k], za_r.at[k], to_z)

    def za_arrival(k):
        return remote(own.at[3 * dp + k], own.at[3 * (1 - dp) + k], za_s.at[k], za_r.at[k], to_z)

    def lanes(core):
        return pl.ds(pl.multiple_of(128 * core, 128), 256)

    f_copy = remote(own.at[:, :, lanes(1 - c)], sums.at[pl.ds(6 * c, 6)], f_s, f_r, to_core)
    f_arrival = remote(own.at[:, :, lanes(1 - c)], sums.at[pl.ds(6 * (1 - c), 6)], f_s, f_r, to_core)

    def convert(k):
        slot = 2 * (k % 2)
        part[k] = stage[slot + 1].astype(BF)
        acc[k] = stage[slot].astype(BF)

    def g_loaded(k):
        g_load(k, 1).wait()
        g_load(k, 0).wait()

    def z_step(k):
        p_copy(3 + k).wait_recv()
        z_copy(k).wait_recv()
        acc[3 + k] = acc[3 + k] + r0[3 + k] + rz[k]

    def d1_send(k):
        d1_copy(k, 0).start()
        d1_copy(k, 1).start()

    def d1_step(k):
        for j in range(2):
            d1_copy(k, j).wait_recv()
        for j in range(2):
            at = pl.ds(BLK * j, BLK)
            kept[k, :, at] = acc[3 + k, :, cols(q_of(j, True))] + r1[k, :, at]

    def d2_step(k):
        d2_copy(k).wait_recv()
        own[3 * dp + k] = kept[k, :, cols(m)] + r2[k]

    def dx_copy(t, size):
        at = pl.ds(pl.multiple_of(t * size, size), size)
        return pltpu.make_async_copy(dxo.at[lax.rem(t, 2)], dx_out.at[:, at], dxo_sem.at[lax.rem(t, 2)])

    dx2_copy = pltpu.make_async_copy(dxa.at[:, pl.ds(2048, TB)], dx2_out, dx2_sem)

    def tile_step(base, size, t, tile, put, parts=1):
        rows = pl.ds(base, size)
        at = pl.ds(pl.multiple_of(t * tile, tile), tile)
        sub = tile // parts
        for j in range(parts):
            ats = pl.ds(pl.multiple_of(t * tile + j * sub, sub), sub)
            cut = slice(j * sub, (j + 1) * sub)
            h_s[:size, cut], da_s[:size, cut], db_s[:size, cut] = forward_tile(xv[:, ats], dv[:, ats], w, rows)
        for j in range(parts):
            cut = slice(j * sub, (j + 1) * sub)
            put(j * sub, sub, dx_tile(da_s[:size, cut], db_s[:size, cut], w, rows))
        xt, dyt = xv[:, at], dv[:, at]
        h, da, db = h_s[:size, :tile], da_s[:size, :tile], db_s[:size, :tile]
        dwa[0, :, rows] += dot(xt, da, NT)
        dwa[1, :, rows] += dot(xt, db, NT)
        dwa[2, :, rows] += dot(dyt, h, NT)

    for n in (0, 2, 4):
        w_load(n).wait()
    w_send(0, 1, 2)
    for n in (1, 3, 5):
        w_load(n).wait()
    w_send(3, 4, 5)
    g_loaded(0)
    convert(0)
    g_load(2, 1).start()
    g_load(2, 0).start()
    p_copy(0).start()
    w_arrived(0)

    def add_partner(k):
        p_copy(k).wait_recv()
        acc[k] = acc[k] + r0[k]

    @pl.loop(0, T // 1024)
    def _(t):
        @pl.when(t < 3)
        def _():
            t_load(t, 0).start()
            t_load(t, 1).start()

        @pl.when(t == 1)
        def _():
            dx2_copy.start()

        @pl.when(t > 0)
        def _():
            add_partner(t - 1)
            p_copy(t).start()
            g_load(t + 2, 1).start()
            g_load(t + 2, 0).start()
            z_copy(t - 1).start()

        @pl.when(t == 3)
        def _():
            dx2_copy.wait()
            w_arrived(1, 2)
            w_send(6, 7, 10)

        tt = lax.rem(t + 3, 4)
        t_load(tt, 0).wait()
        t_load(tt, 1).wait()
        g_loaded(t + 1)
        convert(t + 1)

        def put(off, sub, dx):
            dxa[:, pl.ds(pl.multiple_of(1024 * lax.rem(t + 2, 3) + off, 256), sub)] = dx

        tile_step(0, 256, tt, 1024, put, 4)

    p_copy(4).start()
    g_loaded(5)
    convert(5)
    w_arrived(6, 7)

    @pl.loop(0, TA // 1024)
    def _(t):
        @pl.when(t == 1)
        def _():
            w_arrived(3, 4, 5)
            w_send(8, 9, 11)
            p_copy(5).start()

        @pl.when(t == 2)
        def _():
            w_arrived(10, 11)
            w_send(12, 13)
            z_step(0)
            d1_send(0)

        def put(off, sub, dx):
            dxa[:, pl.ds(pl.multiple_of(1024 * t + off, 256), sub)] += dx

        tile_step(256, 512, t, 1024, put, 4)

    d1_step(0)
    z_step(1)
    d2_copy(0).start()
    d1_send(1)
    w_arrived(8, 9, 12, 13)

    def at_1():
        d2_step(0)
        z_step(2)
        za_copy(0).start()
        d1_send(2)

    def at_2():
        d1_step(1)
        d2_copy(1).start()

    def at_3():
        d2_step(1)
        d1_step(2)
        za_copy(1).start()
        d2_copy(2).start()

    def at_4():
        d2_step(2)
        za_copy(2).start()

    def at_5():
        for k in range(3):
            za_arrival(k).wait_recv()
        f_copy.start()
        sums[pl.ds(6 * c, 6)] = own[:, :, lanes(c)]

    @pl.loop(0, TA // 512)
    def _(t):
        for i, step in ((1, at_1), (2, at_2), (3, at_3), (4, at_4), (5, at_5)):
            pl.when(t == i)(step)

        @pl.when(t >= 2)
        def _():
            dx_copy(t - 2, 512).wait()

        def put(off, sub, dx):
            dxo[lax.rem(t, 2)] = (dxa[:, pl.ds(pl.multiple_of(512 * t, 512), 512)] + dx).astype(BF)

        tile_step(768, 768, t, 512, put)

        @pl.when(t < TA // 512 - 2)
        def _():
            dx_copy(t, 512).start()

    f_arrival.wait_recv()
    for n in range(14):
        w_copy(n).wait_send()
    for k in range(6):
        p_copy(k).wait_send()
    for k in range(3):
        z_copy(k).wait_send()
        d1_copy(k, 0).wait_send()
        d1_copy(k, 1).wait_send()
        d2_copy(k).wait_send()
        za_copy(k).wait_send()
    f_copy.wait_send()


def kernel_b(
    xv, dv, w, dwp, sums, dxo_a, dxp_hbm, dx2_hbm,
    dx_out, dw_out, dn_out,
    dwa, dxp, dx2, flip, dn, da_s, db_s, h_s, dxa, dxo,
    misc_sem, dw_sem, last_sem,
):
    row = lax.axis_index("row")
    f = lax.axis_index("fsdp")
    c = lax.rem(f, 2)
    x = f // 2
    q_own, q_x, q_y, q_d = 2 * row + x, 2 * row + 1 - x, 2 * (1 - row) + x, 2 * (1 - row) + 1 - x
    granule = [3 * q + j for q, j in (
        (q_own, 0), (q_own, 2), (q_x, 0), (q_x, 2), (q_y, 0), (q_y, 2), (q_own, 1), (q_x, 1), (q_y, 1), (q_d, 0), (q_d, 1), (q_d, 2)
    )]

    dxp_load = pltpu.make_async_copy(dxp_hbm, dxp, misc_sem.at[0])
    dxp_store = pltpu.make_async_copy(dxp, dx_out.at[:, pl.ds(0, TA - 1024)], misc_sem.at[1])
    dx2_load = pltpu.make_async_copy(dx2_hbm, dx2, misc_sem.at[2])
    dx_store = pltpu.make_async_copy(dxo, dx_out.at[:, pl.ds(TA, TB)], misc_sem.at[3])
    dn_store = pltpu.make_async_copy(dn, dn_out, misc_sem.at[4])

    def tail_store(i):
        return pltpu.make_async_copy(dxo_a.at[i], dx_out.at[:, pl.ds(TA - 1024 + 512 * i, 512)], misc_sem.at[5 + i])

    def place(k):
        return pl.ds(pl.multiple_of(128 * granule[k], 128), 128)

    def dw_copy(k):
        src = dwp if k < 2 else dwa
        return pltpu.make_async_copy(src.at[:, :, pl.ds(128 * k, 128)], dw_out.at[:, :, place(k)], dw_sem.at[k])

    def last_copy(i, k):
        return pltpu.make_async_copy(dwa.at[i, :, pl.ds(128 * k, 128)], dw_out.at[i, :, place(k)], last_sem.at[i, k - 2])

    for k in range(2):
        dw_copy(k).start()
    dxp_load.start()
    dx2_load.start()
    tail_store(0).start()
    tail_store(1).start()

    rows = pl.ds(768, 768)
    for t in range(2):
        mine, at = pl.ds(TA + 512 * t, 512), pl.ds(512 * t, 512)
        xt, dyt = xv[:, mine], dv[:, mine]
        h_s[:, :512], da_s[:, :512], db_s[:, :512] = forward_tile(xt, dyt, w, rows)
        h, da, db = h_s[:, :512], da_s[:, :512], db_s[:, :512]
        dxa[:, at] = dx_tile(da, db, w, rows)
        for i, (lhs, rhs) in enumerate(((xt, da), (xt, db), (dyt, h))):
            dwa[i, :, rows] = (dwp if t == 0 else dwa)[i, :, rows] + dot(lhs, rhs, NT)
    for k in range(6, 12):
        dw_copy(k).start()
    dxp_load.wait()
    dxp_store.start()
    dx2_load.wait()

    rows = pl.ds(256, 512)
    xt, dyt = xv[:, TA:], dv[:, TA:]
    for i in range(3):
        flip[i] = jnp.transpose(sums[4 * i : 4 * i + 4].reshape(D, 256).astype(F32))
        dn[i] = flip[i, pl.ds(pl.multiple_of(64 * c, 64), 192), :]
    cuts = [slice(j, j + 256) for j in range(0, TB, 256)]
    for cut in cuts:
        h_s[:512, cut], da_s[:512, cut], db_s[:512, cut] = forward_tile(xt[:, cut], dyt[:, cut], w, rows)
    for cut in cuts:
        dxo[:, cut] = (dxa[:, cut] + dx2[:, cut] + dx_tile(da_s[:512, cut], db_s[:512, cut], w, rows)).astype(BF)
    h, da, db = h_s[:512], da_s[:512], db_s[:512]
    dx_store.start()
    dn_store.start()
    for i, (lhs, rhs) in enumerate(((xt, da), (xt, db), (dyt, h))):
        dwa[i, :, rows] = dwp[i, :, rows] + dot(lhs, rhs, NT)
        for k in range(2, 6):
            last_copy(i, k).start()

    for k in (0, 1, 6, 7, 8, 9, 10, 11):
        dw_copy(k).wait()
    dxp_store.wait()
    tail_store(0).wait()
    tail_store(1).wait()
    dx_store.wait()
    dn_store.wait()
    for i in range(3):
        for k in range(2, 6):
            last_copy(i, k).wait()


def per_device(x_blk, dy_blk, gate_shard, up_shard, down_shard, g_part):
    dma = pltpu.SemaphoreType.DMA
    vm, hbm = pltpu.VMEM, pltpu.HBM
    shape = jax.ShapeDtypeStruct
    *in_vmem, dx_part, dx2_part = pl.pallas_call(
        kernel_a,
        out_shape=(
            vm((D, T), BF), vm((D, T), BF), vm((3, H, D), BF), vm((3, D, H), F32), vm((12, CH, 256), BF), vm((2, D, 512), BF), hbm((D, TA - 1024), BF), hbm((D, TB), F32)
        ),
        in_specs=[ANY] * 6,
        out_specs=(VM,) * 6 + (ANY,) * 2,
        scratch_shapes=[
            vm((768, 1024), BF), vm((768, 1024), BF), vm((768, 1024), BF), vm((D, TA), F32),
            vm((4, CH, H), F32), vm((6, CH, H), BF), vm((6, CH, H), BF), vm((6, CH, H), BF), vm((3, CH, H), BF),
            vm((3, CH, 2 * BLK), BF), vm((3, CH, 2 * BLK), BF), vm((3, CH, BLK), BF), vm((6, CH, BLK), BF),
            dma((T // 512,)), dma((6,)), dma((14,)), dma((14,)), dma((4,)), dma((6,)), dma((6,)), dma((3,)), dma((3,)),
            dma((3, 2)), dma((3, 2)), dma((3,)), dma((3,)), dma((3,)), dma((3,)), dma, dma, dma((2,)), dma,
        ],
        compiler_params=pltpu.CompilerParams(collective_id=0, has_side_effects=True, vmem_limit_bytes=VMEM_A),
        name="gather_reduce_backward",
    )(x_blk.T, dy_blk.T, gate_shard.T, up_shard.T, down_shard, g_part.reshape(3 * D, H))
    in_vmem = [pltpu.with_memory_space_constraint(v, pltpu.VMEM) for v in in_vmem]
    dx_t, dw_local, dn_t = pl.pallas_call(
        kernel_b,
        out_shape=(shape((D, T), BF), shape((3, D, H), F32), shape((3, 192, D), F32)),
        in_specs=[VM] * 6 + [ANY] * 2,
        out_specs=(ANY,) * 3,
        scratch_shapes=[
            vm((3, D, H), F32), vm((D, TA - 1024), BF), vm((D, TB), F32), vm((3, 256, D), F32), vm((3, 192, D), F32),
            vm((768, TB), BF), vm((768, TB), BF), vm((768, TB), BF), vm((D, TB), F32), vm((D, TB), BF),
            dma((7,)), dma((12,)), dma((3, 4)),
        ],
        compiler_params=pltpu.CompilerParams(vmem_limit_bytes=VMEM_B),
        name="finish_backward",
    )(*in_vmem, dx_part, dx2_part)
    return dx_t.T, jnp.swapaxes(dn_t, 1, 2), dw_local[None]


def solution(mesh):
    return jax.shard_map(
        per_device,
        mesh=mesh,
        in_specs=(P(ALL_AXES, None), P(ALL_AXES, None), P(None, GROUP_AXES), P(None, GROUP_AXES), P(GROUP_AXES, None), P(ALL_AXES, None, None, None)),
        out_specs=(P(ALL_AXES, None), P(None, None, GROUP_AXES), P(ALL_AXES, None, None, None)),
        check_vma=False,
    )
```

```python
import jax
import jax.numpy as jnp
from jax import lax
from jax.experimental import pallas as pl
from jax.experimental.pallas import tpu as pltpu
from jax.sharding import PartitionSpec as P

ALL_AXES = ("dp", "row", "fsdp")
GROUP_AXES = ("row", "fsdp")
MESH = pl.DeviceIdType.MESH
NN = (((1,), (0,)), ((), ()))
NT = (((1,), (1,)), ((), ()))
TN = (((0,), (0,)), ((), ()))
F32 = jnp.float32
BF = jnp.bfloat16
ANY = pl.BlockSpec(memory_space=pl.ANY)
VM = pl.BlockSpec(memory_space=pltpu.VMEM)

D = 576
H = 1536
T = 4096
TA = 3072
TB = T - TA
CH = 144
BLK = 384
VMEM_A = 37 * 2**20
VMEM_B = 37 * 2**20
OWN_OUT, X_OUT, Y_OUT, OWN_MID, X_MID, Y_MID, DIAG = 0, 256, 512, 768, 896, 1024, 1152


def dot(lhs, rhs, dims):
    return lax.dot_general(lhs, rhs, dims, preferred_element_type=F32)


def forward_tile(x, dy, w, rows):
    a = dot(w[0, rows, :], x, NN)
    b = dot(w[1, rows, :], x, NN)
    dh = dot(w[2, rows, :], dy, NN)
    s = jax.nn.sigmoid(a)
    silu = a * s
    h = (silu * b).astype(BF)
    da = (dh * b * s * (1.0 + a * (1.0 - s))).astype(BF)
    db = (dh * silu).astype(BF)
    return h, da, db


def dx_tile(da, db, w, rows):
    return dot(w[0, rows, :], da, TN) + dot(w[1, rows, :], db, TN)


def kernel_a(
    x_hbm, dy_hbm, w1_hbm, w3_hbm, w2_hbm, g_hbm,
    xv, dv, w, dwa, sums, dxo, dx_out, dx2_out,
    da_s, db_s, h_s, dxa,
    stage, part, r0, acc, rz, r1, kept, r2, own,
    in_sem, wl_sem, ws, wr, st_sem, p_s, p_r, z_s, z_r, d1_s, d1_r, d2_s, d2_r, za_s, za_r, f_s, f_r, dxo_sem, dx2_sem,
):
    dp = lax.axis_index("dp")
    row = lax.axis_index("row")
    f = lax.axis_index("fsdp")
    c = lax.rem(f, 2)
    x = f // 2
    fx = lax.rem(f + 2, 4)
    to_core = {"fsdp": f + 1 - 2 * c}
    to_x = {"fsdp": fx}
    to_y = {"row": 1 - row}
    to_z = {"dp": 1 - dp}
    to_xy = {"row": row + (1 - c) * (1 - 2 * row), "fsdp": f + c * (fx - f)}
    to_first = {"row": row + c * (1 - 2 * row), "fsdp": f + (1 - c) * (fx - f)}

    out_l, mid_l = 64 * c, 128 * (1 - c)

    def w_load(n):
        i, mid = n // 2, n % 2
        src = (w1_hbm, w3_hbm, w2_hbm)[i]
        if mid:
            return pltpu.make_async_copy(
                src.at[pl.ds(pl.multiple_of(mid_l, 64), 64), :], w.at[i, pl.ds(pl.multiple_of(OWN_MID + 64 * c, 64), 64), :], wl_sem.at[n]
            )
        return pltpu.make_async_copy(
            src.at[pl.ds(pl.multiple_of(out_l, 64), 128), :], w.at[i, pl.ds(pl.multiple_of(OWN_OUT + 128 * c, 128), 128), :], wl_sem.at[n]
        )

    def g_load(k, side):
        late = k // 3
        half = (1 - late) * (1 - dp) + late * dp
        core = c if side == 0 else 1 - c
        rows = pl.ds(pl.multiple_of(864 * core + 432 * half + CH * (k % 3), 16), CH)
        slot = 2 * (k % 2) + side
        return pltpu.make_async_copy(g_hbm.at[rows, :], stage.at[slot], st_sem.at[slot])

    def t_load(t, which):
        src, dst = ((x_hbm, xv), (dy_hbm, dv))[which]
        cols = pl.ds(pl.multiple_of(t * 1024, 1024), 1024)
        return pltpu.make_async_copy(src.at[:, cols], dst.at[:, cols], in_sem.at[2 * t + which])

    for n in (0, 2, 4, 1, 3, 5):
        w_load(n).start()
    t_load(3, 0).start()
    t_load(3, 1).start()
    for k in range(2):
        g_load(k, 1).start()
        g_load(k, 0).start()

    barrier = pltpu.get_barrier_semaphore()
    for peer in (to_core, to_x, to_y, to_z):
        pl.semaphore_signal(barrier, inc=1, device_id=peer, device_id_type=MESH)
    pl.semaphore_wait(barrier, 4)

    def w_rows(base, size):
        return w.at[:, pl.ds(pl.multiple_of(base, 64), size), :]

    def w_copy(n):
        o, m = 128 * c, 64 * c
        src, dst, size, peer = (
            (OWN_OUT + o, OWN_OUT + o, 128, to_core),
            (OWN_OUT + o, X_OUT + o, 128, to_x),
            (OWN_OUT + o, Y_OUT + o, 128, to_y),
            (OWN_MID + m, OWN_MID + m, 64, to_core),
            (OWN_MID + m, X_MID + m, 64, to_x),
            (OWN_MID + m, Y_MID + m, 64, to_y),
            (X_OUT + o, X_OUT + o, 128, to_core),
            (Y_OUT + o, Y_OUT + o, 128, to_core),
            (X_MID + m, X_MID + m, 64, to_core),
            (Y_MID + m, Y_MID + m, 64, to_core),
            (X_OUT + c * (Y_OUT + 128 - X_OUT), DIAG + 256 * c, 128, to_xy),
            (X_MID + c * (Y_MID + 64 - X_MID), DIAG + 128 + m, 64, to_xy),
            (DIAG + 256 * c, DIAG + 256 * c, 128, to_core),
            (DIAG + 128 + m, DIAG + 128 + m, 64, to_core),
        )[n]
        return pltpu.make_async_remote_copy(
            src_ref=w_rows(src, size), dst_ref=w_rows(dst, size), send_sem=ws.at[n], recv_sem=wr.at[n], device_id=peer, device_id_type=MESH
        )

    def w_send(*ns):
        for n in ns:
            w_copy(n).start()

    def w_arrived(*ns):
        for n in ns:
            w_copy(n).wait_recv()

    def remote(src, dst, s, r, peer):
        return pltpu.make_async_remote_copy(src_ref=src, dst_ref=dst, send_sem=s, recv_sem=r, device_id=peer, device_id_type=MESH)

    def p_copy(k):
        return remote(part.at[k], r0.at[k], p_s.at[k], p_r.at[k], to_core)

    def z_copy(k):
        return remote(acc.at[k], rz.at[k], z_s.at[k], z_r.at[k], to_z)

    def cols(q):
        return pl.ds(pl.multiple_of(q * BLK, BLK), BLK)

    def q_of(j, mine):
        on_x = 2 * j + (x if mine else 1 - x)
        on_y = 2 * (row if mine else 1 - row) + j
        return (1 - c) * on_x + c * on_y

    def d1_copy(k, j):
        return remote(acc.at[3 + k, :, cols(q_of(j, False))], r1.at[k, :, pl.ds(BLK * j, BLK)], d1_s.at[k, j], d1_r.at[k, j], to_first)

    m = (1 - c) * row + c * x

    def d2_copy(k):
        return remote(kept.at[k, :, cols(1 - m)], r2.at[k], d2_s.at[k], d2_r.at[k], to_xy)

    def za_copy(k):
        return remote(own.at[3 * dp + k], own.at[3 * dp + k], za_s.at[k], za_r.at[k], to_z)

    def za_arrival(k):
        return remote(own.at[3 * dp + k], own.at[3 * (1 - dp) + k], za_s.at[k], za_r.at[k], to_z)

    def lanes(core):
        return pl.ds(pl.multiple_of(128 * core, 128), 256)

    f_copy = remote(own.at[:, :, lanes(1 - c)], sums.at[pl.ds(6 * c, 6)], f_s, f_r, to_core)
    f_arrival = remote(own.at[:, :, lanes(1 - c)], sums.at[pl.ds(6 * (1 - c), 6)], f_s, f_r, to_core)

    def convert(k):
        slot = 2 * (k % 2)
        part[k] = stage[slot + 1].astype(BF)
        acc[k] = stage[slot].astype(BF)

    def g_loaded(k):
        g_load(k, 1).wait()
        g_load(k, 0).wait()

    def z_step(k):
        p_copy(3 + k).wait_recv()
        z_copy(k).wait_recv()
        acc[3 + k] = acc[3 + k] + r0[3 + k] + rz[k]

    def d1_send(k):
        d1_copy(k, 0).start()
        d1_copy(k, 1).start()

    def d1_step(k):
        for j in range(2):
            d1_copy(k, j).wait_recv()
        for j in range(2):
            at = pl.ds(BLK * j, BLK)
            kept[k, :, at] = acc[3 + k, :, cols(q_of(j, True))] + r1[k, :, at]

    def d2_step(k):
        d2_copy(k).wait_recv()
        own[3 * dp + k] = kept[k, :, cols(m)] + r2[k]

    def dx_copy(t, size):
        at = pl.ds(pl.multiple_of(t * size, size), size)
        return pltpu.make_async_copy(dxo.at[lax.rem(t, 2)], dx_out.at[:, at], dxo_sem.at[lax.rem(t, 2)])

    dx2_copy = pltpu.make_async_copy(dxa.at[:, pl.ds(2048, TB)], dx2_out, dx2_sem)

    def tile_step(base, size, t, tile, put, parts=1):
        rows = pl.ds(base, size)
        at = pl.ds(pl.multiple_of(t * tile, tile), tile)
        sub = tile // parts
        for j in range(parts):
            ats = pl.ds(pl.multiple_of(t * tile + j * sub, sub), sub)
            cut = slice(j * sub, (j + 1) * sub)
            h_s[:size, cut], da_s[:size, cut], db_s[:size, cut] = forward_tile(xv[:, ats], dv[:, ats], w, rows)
        for j in range(parts):
            cut = slice(j * sub, (j + 1) * sub)
            put(j * sub, sub, dx_tile(da_s[:size, cut], db_s[:size, cut], w, rows))
        xt, dyt = xv[:, at], dv[:, at]
        h, da, db = h_s[:size, :tile], da_s[:size, :tile], db_s[:size, :tile]
        dwa[0, :, rows] += dot(xt, da, NT)
        dwa[1, :, rows] += dot(xt, db, NT)
        dwa[2, :, rows] += dot(dyt, h, NT)

    for n in (0, 2, 4):
        w_load(n).wait()
    w_send(0, 1, 2)
    for n in (1, 3, 5):
        w_load(n).wait()
    w_send(3, 4, 5)
    for i in range(3):
        dwa[i] = jnp.zeros((D, H), F32)
    g_loaded(0)
    convert(0)
    g_load(2, 1).start()
    g_load(2, 0).start()
    p_copy(0).start()
    w_arrived(0)

    def add_partner(k):
        p_copy(k).wait_recv()
        acc[k] = acc[k] + r0[k]

    @pl.loop(0, T // 1024)
    def _(t):
        @pl.when(t < 3)
        def _():
            t_load(t, 0).start()
            t_load(t, 1).start()

        @pl.when(t == 1)
        def _():
            dx2_copy.start()

        @pl.when(t > 0)
        def _():
            add_partner(t - 1)
            p_copy(t).start()
            g_load(t + 2, 1).start()
            g_load(t + 2, 0).start()
            z_copy(t - 1).start()

        @pl.when(t == 3)
        def _():
            dx2_copy.wait()
            w_arrived(1, 2)
            w_send(6, 7, 10)

        tt = lax.rem(t + 3, 4)
        t_load(tt, 0).wait()
        t_load(tt, 1).wait()
        g_loaded(t + 1)
        convert(t + 1)

        def put(off, sub, dx):
            dxa[:, pl.ds(pl.multiple_of(1024 * lax.rem(t + 2, 3) + off, 256), sub)] = dx

        tile_step(0, 256, tt, 1024, put, 4)

    p_copy(4).start()
    g_loaded(5)
    convert(5)
    w_arrived(6, 7)

    @pl.loop(0, TA // 1024)
    def _(t):
        @pl.when(t == 1)
        def _():
            w_arrived(3, 4, 5)
            w_send(8, 9, 11)
            p_copy(5).start()

        @pl.when(t == 2)
        def _():
            w_arrived(10, 11)
            w_send(12, 13)
            z_step(0)
            d1_send(0)

        def put(off, sub, dx):
            dxa[:, pl.ds(pl.multiple_of(1024 * t + off, 256), sub)] += dx

        tile_step(256, 512, t, 1024, put, 4)

    d1_step(0)
    z_step(1)
    d2_copy(0).start()
    d1_send(1)
    w_arrived(8, 9, 12, 13)

    def at_1():
        d2_step(0)
        z_step(2)
        za_copy(0).start()
        d1_send(2)

    def at_2():
        d1_step(1)
        d2_copy(1).start()

    def at_3():
        d2_step(1)
        d1_step(2)
        za_copy(1).start()
        d2_copy(2).start()

    def at_4():
        d2_step(2)
        za_copy(2).start()

    def at_5():
        for k in range(3):
            za_arrival(k).wait_recv()
        f_copy.start()
        sums[pl.ds(6 * c, 6)] = own[:, :, lanes(c)]

    @pl.loop(0, TA // 512)
    def _(t):
        for i, step in ((1, at_1), (2, at_2), (3, at_3), (4, at_4), (5, at_5)):
            pl.when(t == i)(step)

        @pl.when(t >= 2)
        def _():
            dx_copy(t - 2, 512).wait()

        def put(off, sub, dx):
            dxo[lax.rem(t, 2)] = (dxa[:, pl.ds(pl.multiple_of(512 * t, 512), 512)] + dx).astype(BF)

        tile_step(768, 768, t, 512, put)

        @pl.when(t < TA // 512 - 2)
        def _():
            dx_copy(t, 512).start()

    f_arrival.wait_recv()
    for n in range(14):
        w_copy(n).wait_send()
    for k in range(6):
        p_copy(k).wait_send()
    for k in range(3):
        z_copy(k).wait_send()
        d1_copy(k, 0).wait_send()
        d1_copy(k, 1).wait_send()
        d2_copy(k).wait_send()
        za_copy(k).wait_send()
    f_copy.wait_send()


def kernel_b(
    xv, dv, w, dwp, sums, dxo_a, dxp_hbm, dx2_hbm,
    dx_out, dw_out, dn_out,
    dwa, dxp, dx2, flip, dn, da_s, db_s, h_s, dxa, dxo,
    misc_sem, dw_sem, last_sem,
):
    row = lax.axis_index("row")
    f = lax.axis_index("fsdp")
    c = lax.rem(f, 2)
    x = f // 2
    q_own, q_x, q_y, q_d = 2 * row + x, 2 * row + 1 - x, 2 * (1 - row) + x, 2 * (1 - row) + 1 - x
    granule = [3 * q + j for q, j in (
        (q_own, 0), (q_own, 2), (q_x, 0), (q_x, 2), (q_y, 0), (q_y, 2), (q_own, 1), (q_x, 1), (q_y, 1), (q_d, 0), (q_d, 1), (q_d, 2)
    )]

    dxp_load = pltpu.make_async_copy(dxp_hbm, dxp, misc_sem.at[0])
    dxp_store = pltpu.make_async_copy(dxp, dx_out.at[:, pl.ds(0, TA - 1024)], misc_sem.at[1])
    dx2_load = pltpu.make_async_copy(dx2_hbm, dx2, misc_sem.at[2])
    dx_store = pltpu.make_async_copy(dxo, dx_out.at[:, pl.ds(TA, TB)], misc_sem.at[3])
    dn_store = pltpu.make_async_copy(dn, dn_out, misc_sem.at[4])

    def tail_store(i):
        return pltpu.make_async_copy(dxo_a.at[i], dx_out.at[:, pl.ds(TA - 1024 + 512 * i, 512)], misc_sem.at[5 + i])

    def place(k):
        return pl.ds(pl.multiple_of(128 * granule[k], 128), 128)

    def dw_copy(k):
        src = dwp if k < 2 else dwa
        return pltpu.make_async_copy(src.at[:, :, pl.ds(128 * k, 128)], dw_out.at[:, :, place(k)], dw_sem.at[k])

    def last_copy(i, k):
        return pltpu.make_async_copy(dwa.at[i, :, pl.ds(128 * k, 128)], dw_out.at[i, :, place(k)], last_sem.at[i, k - 2])

    for k in range(2):
        dw_copy(k).start()
    dxp_load.start()
    dx2_load.start()
    tail_store(0).start()
    tail_store(1).start()

    rows = pl.ds(768, 768)
    for t in range(2):
        mine, at = pl.ds(TA + 512 * t, 512), pl.ds(512 * t, 512)
        xt, dyt = xv[:, mine], dv[:, mine]
        h_s[:, :512], da_s[:, :512], db_s[:, :512] = forward_tile(xt, dyt, w, rows)
        h, da, db = h_s[:, :512], da_s[:, :512], db_s[:, :512]
        dxa[:, at] = dx_tile(da, db, w, rows)
        for i, (lhs, rhs) in enumerate(((xt, da), (xt, db), (dyt, h))):
            dwa[i, :, rows] = (dwp if t == 0 else dwa)[i, :, rows] + dot(lhs, rhs, NT)
    for k in range(6, 12):
        dw_copy(k).start()
    dxp_load.wait()
    dxp_store.start()
    dx2_load.wait()

    rows = pl.ds(256, 512)
    xt, dyt = xv[:, TA:], dv[:, TA:]
    for i in range(3):
        flip[i] = jnp.transpose(sums[4 * i : 4 * i + 4].reshape(D, 256).astype(F32))
        dn[i] = flip[i, pl.ds(pl.multiple_of(64 * c, 64), 192), :]
    cuts = [slice(j, j + 256) for j in range(0, TB, 256)]
    for cut in cuts:
        h_s[:512, cut], da_s[:512, cut], db_s[:512, cut] = forward_tile(xt[:, cut], dyt[:, cut], w, rows)
    for cut in cuts:
        dxo[:, cut] = (dxa[:, cut] + dx2[:, cut] + dx_tile(da_s[:512, cut], db_s[:512, cut], w, rows)).astype(BF)
    h, da, db = h_s[:512], da_s[:512], db_s[:512]
    dx_store.start()
    dn_store.start()
    for i, (lhs, rhs) in enumerate(((xt, da), (xt, db), (dyt, h))):
        dwa[i, :, rows] = dwp[i, :, rows] + dot(lhs, rhs, NT)
        for k in range(2, 6):
            last_copy(i, k).start()

    for k in (0, 1, 6, 7, 8, 9, 10, 11):
        dw_copy(k).wait()
    dxp_store.wait()
    tail_store(0).wait()
    tail_store(1).wait()
    dx_store.wait()
    dn_store.wait()
    for i in range(3):
        for k in range(2, 6):
            last_copy(i, k).wait()


def per_device(x_blk, dy_blk, gate_shard, up_shard, down_shard, g_part):
    dma = pltpu.SemaphoreType.DMA
    vm, hbm = pltpu.VMEM, pltpu.HBM
    shape = jax.ShapeDtypeStruct
    *in_vmem, dx_part, dx2_part = pl.pallas_call(
        kernel_a,
        out_shape=(
            vm((D, T), BF), vm((D, T), BF), vm((3, H, D), BF), vm((3, D, H), F32), vm((12, CH, 256), BF), vm((2, D, 512), BF), hbm((D, TA - 1024), BF), hbm((D, TB), F32)
        ),
        in_specs=[ANY] * 6,
        out_specs=(VM,) * 6 + (ANY,) * 2,
        scratch_shapes=[
            vm((768, 1024), BF), vm((768, 1024), BF), vm((768, 1024), BF), vm((D, TA), F32),
            vm((4, CH, H), F32), vm((6, CH, H), BF), vm((6, CH, H), BF), vm((6, CH, H), BF), vm((3, CH, H), BF),
            vm((3, CH, 2 * BLK), BF), vm((3, CH, 2 * BLK), BF), vm((3, CH, BLK), BF), vm((6, CH, BLK), BF),
            dma((T // 512,)), dma((6,)), dma((14,)), dma((14,)), dma((4,)), dma((6,)), dma((6,)), dma((3,)), dma((3,)),
            dma((3, 2)), dma((3, 2)), dma((3,)), dma((3,)), dma((3,)), dma((3,)), dma, dma, dma((2,)), dma,
        ],
        compiler_params=pltpu.CompilerParams(collective_id=0, has_side_effects=True, vmem_limit_bytes=VMEM_A),
        name="gather_reduce_backward",
    )(x_blk.T, dy_blk.T, gate_shard.T, up_shard.T, down_shard, g_part.reshape(3 * D, H))
    in_vmem = [pltpu.with_memory_space_constraint(v, pltpu.VMEM) for v in in_vmem]
    dx_t, dw_local, dn_t = pl.pallas_call(
        kernel_b,
        out_shape=(shape((D, T), BF), shape((3, D, H), F32), shape((3, 192, D), F32)),
        in_specs=[VM] * 6 + [ANY] * 2,
        out_specs=(ANY,) * 3,
        scratch_shapes=[
            vm((3, D, H), F32), vm((D, TA - 1024), BF), vm((D, TB), F32), vm((3, 256, D), F32), vm((3, 192, D), F32),
            vm((768, TB), BF), vm((768, TB), BF), vm((768, TB), BF), vm((D, TB), F32), vm((D, TB), BF),
            dma((7,)), dma((12,)), dma((3, 4)),
        ],
        compiler_params=pltpu.CompilerParams(vmem_limit_bytes=VMEM_B),
        name="finish_backward",
    )(*in_vmem, dx_part, dx2_part)
    return dx_t.T, jnp.swapaxes(dn_t, 1, 2), dw_local[None]


def solution(mesh):
    return jax.shard_map(
        per_device,
        mesh=mesh,
        in_specs=(P(ALL_AXES, None), P(ALL_AXES, None), P(None, GROUP_AXES), P(None, GROUP_AXES), P(GROUP_AXES, None), P(ALL_AXES, None, None, None)),
        out_specs=(P(ALL_AXES, None), P(None, None, GROUP_AXES), P(ALL_AXES, None, None, None)),
        check_vma=False,
    )
```
